32 devices in a mesh: data: 1 (over z), pp: 4 (over y), ep: 8 (over x, core).
Axes of the slice: x: 4, y: 4, z: 1, core: 2. Of those that a mesh axis runs over, the one named last changes fastest.
The devices are a block of a 4x4x8 slice.
Arguments:
- expert_out: bfloat16 [4, 64, 256, 3584], P(('data', 'pp'), 'ep')
- expert_ids: int32 [4, 8, 192, 8], P(('data', 'pp'), 'ep')
- slot_ids: int32 [4, 8, 192, 8], P(('data', 'pp'), 'ep')
- gate_vals: float32 [4, 8, 192, 8], P(('data', 'pp'), 'ep')
- residual: bfloat16 [4, 8, 192, 3584], P(('data', 'pp'), 'ep')
- norm_scale: float32 [4, 3584], P('pp')
- w_query: bfloat16 [4, 3584, 28, 128], P('pp')
- w_key: bfloat16 [4, 3584, 28, 128], P('pp')
- w_value: bfloat16 [4, 3584, 28, 128], P('pp')
- w_out: bfloat16 [4, 28, 128, 3584], P('pp')
Outputs:
- output: bfloat16 [4, 8, 192, 3584], P(('data', 'pp'), 'ep')
All inputs are finite; a program needn't handle non-finite values.
Results may differ from the reference program's by a relative error of at most 0.02.
Values are sent between devices in bfloat16 or wider.
A program may use at most 768 MiB of HBM per device.

```python
import jax
import jax.numpy as jnp
from jax import lax

STAGES = 4
EP_DEVS = 8
SEQS_DEV = 1
SEQ_LEN = 192
D = 3584
HEADS = 28
HEAD = 128
EXPERTS = 64
TOP = 8
CAP_DEV = 32

NUM_SEQ = EP_DEVS * SEQS_DEV
TOKENS = NUM_SEQ * SEQ_LEN
TOK_DEV = SEQS_DEV * SEQ_LEN
CAPACITY = EP_DEVS * CAP_DEV
HIDDEN = HEADS * HEAD
NORM_EPS = 1e-6


def queue_pos(flat_ids):
    sort_order = jnp.argsort(flat_ids, stable=True)
    ordered = flat_ids[sort_order]
    first_pos = jnp.searchsorted(ordered, ordered, side='left')
    rank_sorted = jnp.arange(flat_ids.shape[0]) - first_pos
    return rank_sorted[jnp.argsort(sort_order, stable=True)]


def draw_routing(route_key):
    rank_key, noise_key = jax.random.split(route_key)
    rank_draw = jax.random.randint(rank_key, (STAGES, EXPERTS), 0, 1 << 20) * EXPERTS + jnp.arange(EXPERTS)
    expert_rank = jnp.argsort(rank_draw, axis=-1)
    hot_bias = jnp.where(expert_rank == 0, 4000, jnp.where(expert_rank < 3, 200, 0))
    stage_keys = jax.random.split(noise_key, STAGES)

    def pick_stage(stage_args):
        stage_key, stage_bias = stage_args
        score_noise = jax.random.randint(stage_key, (TOKENS, EXPERTS), 0, 1000)
        score_total = (score_noise + stage_bias) * EXPERTS + jnp.arange(EXPERTS)
        return lax.top_k(score_total, TOP)[1]

    expert_ids = lax.map(pick_stage, (stage_keys, hot_bias)).astype(jnp.int32)
    positions = jax.vmap(queue_pos)(expert_ids.reshape(STAGES * EP_DEVS, TOK_DEV * TOP))
    positions = positions.reshape(STAGES, NUM_SEQ, SEQ_LEN, TOP)
    owner_dev = (jnp.arange(NUM_SEQ) // SEQS_DEV)[None, :, None, None]
    slot_ids = jnp.where(positions < CAP_DEV, owner_dev * CAP_DEV + positions, -1).astype(jnp.int32)
    return expert_ids.reshape(STAGES, NUM_SEQ, SEQ_LEN, TOP), slot_ids


def setup_inputs(seed: int = 0, part: int = 0) -> dict:
    base_key = jax.random.key(seed)
    part_key = jax.random.fold_in(base_key, part)
    route_key, out_key, gain_key, mean_key, gate_key, resid_key = jax.random.split(part_key, 6)
    norm_key, q_key, k_key, v_key, o_key = jax.random.split(base_key, 5)
    expert_ids, slot_ids = draw_routing(route_key)
    expert_gain = jnp.exp(0.6 * jax.random.normal(gain_key, (STAGES, EXPERTS, 1, 1), jnp.float32))
    expert_mean = 0.7 * jax.random.normal(mean_key, (STAGES, EXPERTS, 1, D), jnp.float32)
    expert_out = (expert_mean + expert_gain * jax.random.normal(out_key, (STAGES, EXPERTS, CAPACITY, D), jnp.float32)).astype(jnp.bfloat16)
    gate_vals = jax.nn.softmax(2.0 * jax.random.normal(gate_key, (STAGES, NUM_SEQ, SEQ_LEN, TOP), jnp.float32), axis=-1).astype(jnp.float32)
    residual = jax.random.normal(resid_key, (STAGES, NUM_SEQ, SEQ_LEN, D), jnp.float32).astype(jnp.bfloat16)
    norm_scale = jnp.exp(0.5 * jax.random.normal(norm_key, (STAGES, D), jnp.float32)).astype(jnp.float32)
    w_query = (1.3 * D ** -0.5 * jax.random.normal(q_key, (STAGES, D, HEADS, HEAD), jnp.float32)).astype(jnp.bfloat16)
    w_key = (1.3 * D ** -0.5 * jax.random.normal(k_key, (STAGES, D, HEADS, HEAD), jnp.float32)).astype(jnp.bfloat16)
    w_value = (D ** -0.5 * jax.random.normal(v_key, (STAGES, D, HEADS, HEAD), jnp.float32)).astype(jnp.bfloat16)
    w_out = (3.0 * HIDDEN ** -0.5 * jax.random.normal(o_key, (STAGES, HEADS, HEAD, D), jnp.float32)).astype(jnp.bfloat16)
    return {'expert_out': expert_out, 'expert_ids': expert_ids, 'slot_ids': slot_ids, 'gate_vals': gate_vals, 'residual': residual, 'norm_scale': norm_scale, 'w_query': w_query, 'w_key': w_key, 'w_value': w_value, 'w_out': w_out}


def combine_rows(expert_table, ids_seq, slots_seq, gates_seq, resid_seq):
    kept_mask = slots_seq >= 0
    picked_rows = expert_table[ids_seq, jnp.where(kept_mask, slots_seq, 0)].astype(jnp.float32)
    gate_used = jnp.where(kept_mask, gates_seq, 0.0)
    merged = resid_seq.astype(jnp.float32) + jnp.sum(gate_used[..., None] * picked_rows, axis=1)
    return merged.astype(jnp.bfloat16)


def attn_block(merged, scale_vec, q_mat, k_mat, v_mat, o_mat):
    resid_f32 = merged.astype(jnp.float32)
    inv_rms = lax.rsqrt(jnp.mean(resid_f32 * resid_f32, axis=-1, keepdims=True) + NORM_EPS)
    normed_in = (resid_f32 * inv_rms * scale_vec).astype(jnp.bfloat16)

    def project(w_mat):
        product = jnp.dot(normed_in, w_mat, preferred_element_type=jnp.float32).astype(jnp.bfloat16)
        return product.reshape(SEQ_LEN, HEADS, HEAD).astype(jnp.float32)

    q_heads = project(q_mat)
    k_heads = project(k_mat)
    v_heads = project(v_mat)
    scores = jnp.einsum('qhe,khe->hqk', q_heads, k_heads) * HEAD ** -0.5
    causal = jnp.arange(SEQ_LEN)[:, None] >= jnp.arange(SEQ_LEN)[None, :]
    scores = jnp.where(causal, scores, -1e30)
    exp_scores = jnp.exp(scores - jnp.max(scores, axis=-1, keepdims=True))
    row_sums = jnp.sum(exp_scores, axis=-1)
    mixed_vals = jnp.einsum('hqk,khe->qhe', exp_scores.astype(jnp.bfloat16).astype(jnp.float32), v_heads)
    attn_out = (mixed_vals / row_sums.T[:, :, None]).astype(jnp.bfloat16).reshape(SEQ_LEN, HIDDEN)
    proj_out = jnp.dot(attn_out, o_mat, preferred_element_type=jnp.float32).astype(jnp.bfloat16)
    return (resid_f32 + proj_out.astype(jnp.float32)).astype(jnp.bfloat16)


def reference(expert_out, expert_ids, slot_ids, gate_vals, residual, norm_scale, w_query, w_key, w_value, w_out):
    def one_stage(stage_idx):
        prev_stage = (stage_idx + STAGES - 1) % STAGES
        expert_table = expert_out[prev_stage]
        scale_vec = norm_scale[stage_idx]
        q_mat = w_query[stage_idx].reshape(D, HIDDEN)
        k_mat = w_key[stage_idx].reshape(D, HIDDEN)
        v_mat = w_value[stage_idx].reshape(D, HIDDEN)
        o_mat = w_out[stage_idx].reshape(HIDDEN, D)

        def one_seq(seq_idx):
            merged = combine_rows(expert_table, expert_ids[prev_stage, seq_idx], slot_ids[prev_stage, seq_idx], gate_vals[prev_stage, seq_idx], residual[prev_stage, seq_idx])
            return attn_block(merged, scale_vec, q_mat, k_mat, v_mat, o_mat)

        return lax.map(one_seq, jnp.arange(NUM_SEQ))

    return lax.map(one_stage, jnp.arange(STAGES))
```

```python
import functools

import jax
import jax.numpy as jnp
from jax import lax
from jax.experimental import pallas as pl
from jax.experimental.pallas import tpu as pltpu
from jax.sharding import PartitionSpec as P

NORM_EPS = 1e-6
COLS = 256
MESH = pl.DeviceIdType.MESH


def attn_block(merged, scale_vec, w_query, w_key, w_value, w_out):
    head_dim = w_query.shape[-1]
    seq_len = merged.shape[1]
    resid_f32 = merged.astype(jnp.float32)
    inv_rms = lax.rsqrt(jnp.mean(resid_f32 * resid_f32, axis=-1, keepdims=True) + NORM_EPS)
    normed_in = (resid_f32 * inv_rms * scale_vec).astype(jnp.bfloat16)
    q_heads = jnp.einsum('bld,dhe->blhe', normed_in, w_query, preferred_element_type=jnp.float32).astype(jnp.bfloat16)
    k_heads = jnp.einsum('bld,dhe->blhe', normed_in, w_key, preferred_element_type=jnp.float32).astype(jnp.bfloat16)
    v_heads = jnp.einsum('bld,dhe->blhe', normed_in, w_value, preferred_element_type=jnp.float32).astype(jnp.bfloat16)
    scores = jnp.einsum('bqhe,bkhe->bhqk', q_heads, k_heads, preferred_element_type=jnp.float32) * (head_dim ** -0.5)
    causal = jnp.arange(seq_len)[:, None] >= jnp.arange(seq_len)[None, :]
    scores = jnp.where(causal, scores, -1e30)
    exp_scores = jnp.exp(scores - jnp.max(scores, axis=-1, keepdims=True))
    row_sums = jnp.sum(exp_scores, axis=-1)
    mixed_vals = jnp.einsum('bhqk,bkhe->bqhe', exp_scores.astype(jnp.bfloat16), v_heads, preferred_element_type=jnp.float32)
    attn_out = (mixed_vals / jnp.swapaxes(row_sums, -1, -2)[..., None]).astype(jnp.bfloat16)
    proj_out = jnp.einsum('crif,ife->cre', attn_out, w_out, preferred_element_type=jnp.float32).astype(jnp.bfloat16)
    return (resid_f32 + proj_out.astype(jnp.float32)).astype(jnp.bfloat16)


def combine_kernel(sizes, o_hbm, ids, slots, gates, h_hbm, y_out,
                   rows_v, resid_v, meta, gate_mats, send_v, recv_v, ysend_v, y_v,
                   rows_loc, rows_ss, rows_rs, res_loc, res_ss, res_rs, meta_ss, meta_rs,
                   ring_ss, ring_rs, y_ss, y_rs, out_sem):
    ep, pp, experts, cap, width, tokens, top = sizes
    chips = ep // 2
    half = width // 2
    blocks = half // COLS
    cap_dev = cap // ep
    chip_rows = 2 * experts * cap_dev
    me = lax.axis_index('ep')
    stage = lax.axis_index('pp')
    chip, core = me // 2, me % 2
    partner = chip * 2 + (1 - core)
    ahead, behind, across = (chip + 1) % chips, (chip + chips - 1) % chips, (chip + 2) % chips
    next_stage, prev_stage = (stage + 1) % pp, (stage + pp - 1) % pp
    right, left = 2 * ahead + core, 2 * behind + core
    owners = (2 * across, 2 * across + 1, 2 * ahead + 1, 2 * behind, 2 * ahead, 2 * behind + 1, 2 * chip, 2 * chip + 1)

    def local_rows(j):
        cols = pl.ds(pl.multiple_of(core * half + j * COLS, COLS), COLS)
        return pltpu.make_async_copy(o_hbm.at[:, :, cols], rows_v.at[j, pl.ds(core * experts, experts)], rows_loc.at[j])

    def swap_rows(j):
        cols = pl.ds(pl.multiple_of((1 - core) * half + j * COLS, COLS), COLS)
        return pltpu.make_async_remote_copy(
            src_ref=o_hbm.at[:, :, cols], dst_ref=rows_v.at[j, pl.ds(core * experts, experts)],
            send_sem=rows_ss.at[j], recv_sem=rows_rs.at[j], device_id={'ep': partner}, device_id_type=MESH)

    own_cols = pl.ds(pl.multiple_of(core * half, COLS), half)
    other_cols = pl.ds(pl.multiple_of((1 - core) * half, COLS), half)
    local_resid = pltpu.make_async_copy(h_hbm.at[:, own_cols], resid_v.at[core], res_loc)
    swap_resid = pltpu.make_async_remote_copy(
        src_ref=h_hbm.at[:, other_cols], dst_ref=resid_v.at[core],
        send_sem=res_ss, recv_sem=res_rs, device_id={'ep': partner}, device_id_type=MESH)

    def meta_copy(step):
        return pltpu.make_async_remote_copy(
            src_ref=meta.at[me], dst_ref=meta.at[me], send_sem=meta_ss.at[step - 1], recv_sem=meta_rs.at[step - 1],
            device_id={'ep': (me + step) % ep}, device_id_type=MESH)

    def ring_copy(kind, j):
        target = right if kind % 2 == 0 else left
        return pltpu.make_async_remote_copy(
            src_ref=send_v.at[kind, j % 2], dst_ref=recv_v.at[kind, j], send_sem=ring_ss.at[kind, j],
            recv_sem=ring_rs.at[kind, j], device_id={'ep': target}, device_id_type=MESH)

    def y_copy(side, j):
        return pltpu.make_async_remote_copy(
            src_ref=ysend_v.at[side, j % 2], dst_ref=y_v.at[core * blocks + j], send_sem=y_ss.at[side, j],
            recv_sem=y_rs.at[core * blocks + j], device_id={'pp': next_stage, 'ep': 2 * chip + side}, device_id_type=MESH)

    for j in range(blocks):
        local_rows(j).start()
    local_resid.start()
    row_ids = jnp.where(slots[...] >= 0, ids[...] * cap_dev + slots[...] - me * cap_dev, -1)
    meta[me, 0:top, :] = row_ids.astype(jnp.float32)
    meta[me, top:2 * top, :] = gates[...]

    barrier = pltpu.get_barrier_semaphore()
    for step in range(1, ep):
        pl.semaphore_signal(barrier, inc=1, device_id={'ep': (me + step) % ep}, device_id_type=MESH)
    for side in range(2):
        pl.semaphore_signal(barrier, inc=1, device_id={'pp': next_stage, 'ep': 2 * chip + side}, device_id_type=MESH)
        pl.semaphore_signal(barrier, inc=1, device_id={'pp': prev_stage, 'ep': 2 * chip + side}, device_id_type=MESH)
    pl.semaphore_wait(barrier, ep - 1 + 4)

    for step in range(1, ep):
        meta_copy(step).start()
    for j in range(blocks):
        swap_rows(j).start()
    swap_resid.start()

    def build_gates(role):
        table = jnp.transpose(meta[owners[role]])
        wanted = (lax.broadcasted_iota(jnp.int32, (tokens, chip_rows), 1) + chip * chip_rows).astype(jnp.float32)
        total = jnp.zeros((tokens, chip_rows), jnp.float32)
        for t in range(top):
            total = total + jnp.where(table[:, t:t + 1] == wanted, table[:, top + t:top + t + 1], 0.0)
        high = total.astype(jnp.bfloat16)
        rest = total - high.astype(jnp.float32)
        mid = rest.astype(jnp.bfloat16)
        low = (rest - mid.astype(jnp.float32)).astype(jnp.bfloat16)
        gate_mats[role, 0:tokens] = high
        gate_mats[role, tokens:2 * tokens] = mid
        gate_mats[role, 2 * tokens:3 * tokens] = low

    def contribution(role, j):
        slot0 = pl.multiple_of(owners[role] * cap_dev, cap_dev)
        rows = rows_v[j, :, pl.ds(slot0, cap_dev), :].reshape(chip_rows, COLS)
        parts = jnp.dot(gate_mats[role], rows, preferred_element_type=jnp.float32)
        return parts[2 * tokens:] + parts[tokens:2 * tokens] + parts[:tokens]

    def finish(j):
        for side, (near, far) in enumerate(((3, 4), (2, 5))):
            own = contribution(6 + side, j)

            @pl.when(j >= 2)
            def _():
                y_copy(side, j - 2).wait_send()

            ring_copy(near, j).wait_recv()
            ring_copy(far, j).wait_recv()
            cols = pl.ds(pl.multiple_of(j * COLS, COLS), COLS)
            total = resid_v[side, :, cols].astype(jnp.float32) + (own + recv_v[near, j] + recv_v[far, j])
            ysend_v[side, j % 2] = total.astype(jnp.bfloat16)
            y_copy(side, j).start()

    for step in range(1, ep):
        meta_copy(step).wait_recv()

    def block_step(j, carry):
        local_rows(j).wait()
        swap_rows(j).wait_recv()

        for kind in range(4):
            @pl.when(j == 0)
            def _():
                build_gates(kind)

            @pl.when(j >= 2)
            def _():
                ring_copy(kind, j - 2).wait_send()

            send_v[kind, j % 2] = contribution(kind, j)
            ring_copy(kind, j).start()

        @pl.when(j == 0)
        def _():
            for role in range(4, 8):
                build_gates(role)
            local_resid.wait()
            swap_resid.wait_recv()

        @pl.when(j > 0)
        def _():
            finish(j - 1)

        for kind in (4, 5):
            own = contribution(kind, j)

            @pl.when(j >= 2)
            def _():
                ring_copy(kind, j - 2).wait_send()

            ring_copy(kind - 4, j).wait_recv()
            send_v[kind, j % 2] = own + recv_v[kind - 4, j]
            ring_copy(kind, j).start()
        return carry

    lax.fori_loop(0, blocks, block_step, 0)
    finish(blocks - 1)

    def y_arrived(i):
        pltpu.make_async_copy(y_v.at[i], y_v.at[i], y_rs.at[i]).wait()

    def store_out(i):
        return pltpu.make_async_copy(y_v.at[i], y_out.at[:, pl.ds(i * COLS, COLS)], out_sem.at[i])

    for j in range(blocks):
        for side in range(2):
            i = side * blocks + j
            y_arrived(i)
            store_out(i).start()
    for i in range(2 * blocks):
        store_out(i).wait()
    for step in range(1, ep):
        meta_copy(step).wait_send()
    for j in range(blocks):
        swap_rows(j).wait_send()
    swap_resid.wait_send()
    for j in range(blocks - 2, blocks):
        for kind in range(6):
            ring_copy(kind, j).wait_send()
        for side in range(2):
            y_copy(side, j).wait_send()


def combine_and_send(ep, pp, expert_out, expert_ids, slot_ids, gate_vals, residual):
    experts, cap, width = expert_out.shape
    tokens, top = expert_ids.shape
    sizes = (ep, pp, experts, cap, width, tokens, top)
    blocks = width // 2 // COLS
    chip_rows = 2 * experts * cap // ep
    any_spec = pl.BlockSpec(memory_space=pl.ANY)
    vmem_spec = pl.BlockSpec(memory_space=pltpu.VMEM)
    dma = pltpu.SemaphoreType.DMA
    return pl.pallas_call(
        functools.partial(combine_kernel, sizes),
        out_shape=jax.ShapeDtypeStruct((tokens, width), jnp.bfloat16),
        in_specs=[any_spec, vmem_spec, vmem_spec, vmem_spec, any_spec],
        out_specs=any_spec,
        scratch_shapes=[
            pltpu.VMEM((blocks, 2 * experts, cap, COLS), jnp.bfloat16),
            pltpu.VMEM((2, tokens, width // 2), jnp.bfloat16),
            pltpu.VMEM((ep, 2 * top, tokens), jnp.float32),
            pltpu.VMEM((8, 3 * tokens, chip_rows), jnp.bfloat16),
            pltpu.VMEM((6, 2, tokens, COLS), jnp.float32),
            pltpu.VMEM((6, blocks, tokens, COLS), jnp.float32),
            pltpu.VMEM((2, 2, tokens, COLS), jnp.bfloat16),
            pltpu.VMEM((2 * blocks, tokens, COLS), jnp.bfloat16),
            dma((blocks,)), dma((blocks,)), dma((blocks,)), dma, dma, dma, dma((ep - 1,)), dma((ep - 1,)),
            dma((6, blocks)), dma((6, blocks)), dma((2, blocks)), dma((2 * blocks,)), dma((2 * blocks,)),
        ],
        compiler_params=pltpu.CompilerParams(collective_id=0, has_side_effects=True, vmem_limit_bytes=60 * 2 ** 20),
    )(expert_out, expert_ids.T, slot_ids.T, gate_vals.T, residual)


def solution(mesh):
    ep_size = mesh.shape['ep']
    pp_size = mesh.shape['pp']
    token_spec = P(('data', 'pp'), 'ep', None, None)
    weight_spec = P('pp', None, None, None)

    def body(expert_out, expert_ids, slot_ids, gate_vals, residual, norm_scale, w_query, w_key, w_value, w_out):
        arrived = combine_and_send(ep_size, pp_size, expert_out[0], expert_ids[0, 0], slot_ids[0, 0], gate_vals[0, 0], residual[0, 0])
        result = attn_block(arrived[None], norm_scale[0], w_query[0], w_key[0], w_value[0], w_out[0])
        return result[None]

    return jax.shard_map(body, mesh=mesh, in_specs=(token_spec, token_spec, token_spec, token_spec, token_spec, P('pp', None), weight_spec, weight_spec, weight_spec, weight_spec), out_specs=token_spec, check_vma=False)
```

```python
import functools

import jax
import jax.numpy as jnp
from jax import lax
from jax.experimental import pallas as pl
from jax.experimental.pallas import tpu as pltpu
from jax.sharding import PartitionSpec as P

NORM_EPS = 1e-6
COLS = 256
SLOTS = 19
MESH = pl.DeviceIdType.MESH


def layer_kernel(sizes, o_hbm, ids, slots, gates, h_hbm, scale_ref, wq_hbm, wk_hbm, wv_hbm, wo_hbm, z_out,
                 pool, resid_v, meta, gate_mats, send_v, recv_v, ysend_v, y_v, square_v, x_v, qkv_v, mix_v, z_v,
                 rows_loc, rows_ss, rows_rs, res_loc, res_ss, res_rs, meta_ss, meta_rs,
                 ring_ss, ring_rs, y_ss, y_rs, w_sem, z_sem):
    ep, pp, experts, cap, width, tokens, top, heads, head_dim = sizes
    chips = ep // 2
    half = width // 2
    blocks = half // COLS
    cap_dev = cap // ep
    chip_rows = 2 * experts * cap_dev
    me = lax.axis_index('ep')
    stage = lax.axis_index('pp')
    chip, core = me // 2, me % 2
    partner = chip * 2 + (1 - core)
    ahead, behind, across = (chip + 1) % chips, (chip + chips - 1) % chips, (chip + 2) % chips
    next_stage, prev_stage = (stage + 1) % pp, (stage + pp - 1) % pp
    right, left = 2 * ahead + core, 2 * behind + core
    owners = (2 * across, 2 * across + 1, 2 * ahead + 1, 2 * behind, 2 * ahead, 2 * behind + 1, 2 * chip, 2 * chip + 1)

    def local_rows(j):
        cols = pl.ds(pl.multiple_of(core * half + j * COLS, COLS), COLS)
        return pltpu.make_async_copy(o_hbm.at[:, :, cols], pool.at[j, pl.ds(core * experts, experts)], rows_loc.at[j])

    def swap_rows(j):
        cols = pl.ds(pl.multiple_of((1 - core) * half + j * COLS, COLS), COLS)
        return pltpu.make_async_remote_copy(
            src_ref=o_hbm.at[:, :, cols], dst_ref=pool.at[j, pl.ds(core * experts, experts)],
            send_sem=rows_ss.at[j], recv_sem=rows_rs.at[j], device_id={'ep': partner}, device_id_type=MESH)

    own_cols = pl.ds(pl.multiple_of(core * half, COLS), half)
    other_cols = pl.ds(pl.multiple_of((1 - core) * half, COLS), half)
    local_resid = pltpu.make_async_copy(h_hbm.at[:, own_cols], resid_v.at[core], res_loc)
    swap_resid = pltpu.make_async_remote_copy(
        src_ref=h_hbm.at[:, other_cols], dst_ref=resid_v.at[core],
        send_sem=res_ss, recv_sem=res_rs, device_id={'ep': partner}, device_id_type=MESH)

    def meta_copy(step):
        return pltpu.make_async_remote_copy(
            src_ref=meta.at[me], dst_ref=meta.at[me], send_sem=meta_ss.at[step - 1], recv_sem=meta_rs.at[step - 1],
            device_id={'ep': (me + step) % ep}, device_id_type=MESH)

    def ring_copy(kind, j):
        target = right if kind % 2 == 0 else left
        return pltpu.make_async_remote_copy(
            src_ref=send_v.at[kind, j % 2], dst_ref=recv_v.at[kind, j], send_sem=ring_ss.at[kind, j],
            recv_sem=ring_rs.at[kind, j], device_id={'ep': target}, device_id_type=MESH)

    def y_copy(side, j):
        return pltpu.make_async_remote_copy(
            src_ref=ysend_v.at[side, j % 2], dst_ref=y_v.at[core * blocks + j], send_sem=y_ss.at[side, j],
            recv_sem=y_rs.at[core * blocks + j], device_id={'pp': next_stage, 'ep': 2 * chip + side}, device_id_type=MESH)


    pairs = heads // 2
    depth = width // COLS
    n_slots = pool.shape[0]
    early = n_slots - blocks
    units = 3 * pairs + width // COLS

    def qkv_copies(which, pair, slot):
        w_hbm = (wq_hbm, wk_hbm, wv_hbm)[which]
        return [pltpu.make_async_copy(w_hbm.at[2 * pair + i], pool.at[slot, 0:depth, :, i * head_dim:(i + 1) * head_dim],
                                      w_sem.at[slot, i]) for i in range(2)]

    def out_copies(n, slot):
        cols = pl.ds(pl.multiple_of(n * COLS, COLS), COLS)
        mid = depth // 2
        return [pltpu.make_async_copy(wo_hbm.at[i * mid:(i + 1) * mid, :, cols], pool.at[slot, i * mid:(i + 1) * mid],
                                      w_sem.at[slot, i]) for i in range(2)]

    def slot_of(unit):
        return (unit + blocks) % n_slots

    def start_all(copies):
        for copy in copies:
            copy.start()

    def start_unit(unit, which):
        @pl.when(unit < 3 * pairs)
        def _():
            start_all(qkv_copies(which, unit // 3, slot_of(unit)))

        @pl.when(jnp.logical_and(unit >= 3 * pairs, unit < units))
        def _():
            start_all(out_copies(unit - 3 * pairs, slot_of(unit)))

    def start_any(unit):
        for which in range(3):
            @pl.when(unit % 3 == which)
            def _():
                start_unit(unit, which)

    def square_piece(j):
        for side in range(2):
            piece = y_v[side * blocks + j].astype(jnp.float32)
            square_v[...] += piece * piece

    def wait_y(j):
        for side in range(2):
            pltpu.make_async_copy(y_v.at[side * blocks + j], y_v.at[side * blocks + j], y_rs.at[side * blocks + j]).wait()

    for j in range(blocks):
        local_rows(j).start()
    local_resid.start()
    square_v[...] = jnp.zeros_like(square_v)
    row_ids = jnp.where(slots[...] >= 0, ids[...] * cap_dev + slots[...] - me * cap_dev, -1)
    meta[me, 0:top, :] = row_ids.astype(jnp.float32)
    meta[me, top:2 * top, :] = gates[...]

    barrier = pltpu.get_barrier_semaphore()
    for step in range(1, ep):
        pl.semaphore_signal(barrier, inc=1, device_id={'ep': (me + step) % ep}, device_id_type=MESH)
    for side in range(2):
        pl.semaphore_signal(barrier, inc=1, device_id={'pp': next_stage, 'ep': 2 * chip + side}, device_id_type=MESH)
        pl.semaphore_signal(barrier, inc=1, device_id={'pp': prev_stage, 'ep': 2 * chip + side}, device_id_type=MESH)
    pl.semaphore_wait(barrier, ep - 1 + 4)

    for step in range(1, ep):
        meta_copy(step).start()
    for j in range(blocks):
        swap_rows(j).start()
    swap_resid.start()

    def build_gates(role):
        table = jnp.transpose(meta[owners[role]])
        wanted = (lax.broadcasted_iota(jnp.int32, (tokens, chip_rows), 1) + chip * chip_rows).astype(jnp.float32)
        total = jnp.zeros((tokens, chip_rows), jnp.float32)
        for t in range(top):
            total = total + jnp.where(table[:, t:t + 1] == wanted, table[:, top + t:top + t + 1], 0.0)
        high = total.astype(jnp.bfloat16)
        rest = total - high.astype(jnp.float32)
        mid = rest.astype(jnp.bfloat16)
        low = (rest - mid.astype(jnp.float32)).astype(jnp.bfloat16)
        gate_mats[role, 0:tokens] = high
        gate_mats[role, tokens:2 * tokens] = mid
        gate_mats[role, 2 * tokens:3 * tokens] = low

    def contribution(role, j):
        slot0 = pl.multiple_of(owners[role] * cap_dev, cap_dev)
        rows = pool[j, :, pl.ds(slot0, cap_dev), :].reshape(chip_rows, COLS)
        parts = jnp.dot(gate_mats[role], rows, preferred_element_type=jnp.float32)
        return parts[2 * tokens:] + parts[tokens:2 * tokens] + parts[:tokens]

    def finish(j):
        for side, (near, far) in enumerate(((3, 4), (2, 5))):
            own = contribution(6 + side, j)

            @pl.when(j >= 2)
            def _():
                y_copy(side, j - 2).wait_send()

            ring_copy(near, j).wait_recv()
            ring_copy(far, j).wait_recv()
            cols = pl.ds(pl.multiple_of(j * COLS, COLS), COLS)
            total = resid_v[side, :, cols].astype(jnp.float32) + (own + recv_v[near, j] + recv_v[far, j])
            ysend_v[side, j % 2] = total.astype(jnp.bfloat16)
            y_copy(side, j).start()

    for step in range(1, ep):
        meta_copy(step).wait_recv()

    def block_step(j, carry):
        local_rows(j).wait()
        swap_rows(j).wait_recv()

        for kind in range(4):
            @pl.when(j == 0)
            def _():
                build_gates(kind)

            @pl.when(j >= 2)
            def _():
                ring_copy(kind, j - 2).wait_send()

            send_v[kind, j % 2] = contribution(kind, j)
            ring_copy(kind, j).start()

        @pl.when(j == 0)
        def _():
            for role in range(4, 8):
                build_gates(role)
            local_resid.wait()
            swap_resid.wait_recv()
            for unit in range(early):
                start_all(qkv_copies(unit % 3, unit // 3, slot_of(unit)))

        @pl.when(j > 0)
        def _():
            finish(j - 1)
            start_any(early + j - 1)

        @pl.when(j > 1)
        def _():
            wait_y(j - 2)
            square_piece(j - 2)

        for kind in (4, 5):
            own = contribution(kind, j)

            @pl.when(j >= 2)
            def _():
                ring_copy(kind, j - 2).wait_send()

            ring_copy(kind - 4, j).wait_recv()
            send_v[kind, j % 2] = own + recv_v[kind - 4, j]
            ring_copy(kind, j).start()
        return carry

    lax.fori_loop(0, blocks, block_step, 0)
    finish(blocks - 1)

    start_any(early + blocks - 1)
    for j in (blocks - 2, blocks - 1):
        wait_y(j)
        square_piece(j)
    mean = jnp.sum(square_v[...], axis=-1, keepdims=True) / width
    inv_rms = lax.rsqrt(mean + NORM_EPS)
    for i in range(depth):
        cols = slice(i * COLS, (i + 1) * COLS)
        x_v[:, cols] = (y_v[i].astype(jnp.float32) * inv_rms * scale_ref[:, cols]).astype(jnp.bfloat16)

    def wait_unit(unit):
        for copy in out_copies(0, slot_of(unit)):
            copy.wait()

    def weight(unit):
        return pool[slot_of(unit), 0:depth].reshape(width, COLS)

    def project(pair):
        for which in range(3):
            product = jnp.dot(x_v[...], weight(3 * pair + which), preferred_element_type=jnp.float32)
            qkv_v[pair % 2, which] = product.astype(jnp.bfloat16)

    causal = lax.broadcasted_iota(jnp.int32, (tokens, tokens), 0) >= lax.broadcasted_iota(jnp.int32, (tokens, tokens), 1)

    def attend(pair):
        mixed = []
        for i in range(2):
            lanes = slice(i * head_dim, (i + 1) * head_dim)
            q, k, v = (qkv_v[pair % 2, which, :, lanes] for which in range(3))
            scores = lax.dot_general(q, k, (((1,), (1,)), ((), ())), preferred_element_type=jnp.float32) * head_dim ** -0.5
            scores = jnp.where(causal, scores, -1e30)
            exps = jnp.exp(scores - jnp.max(scores, axis=-1, keepdims=True))
            sums = jnp.sum(exps, axis=-1, keepdims=True)
            mixed.append((jnp.dot(exps.astype(jnp.bfloat16), v, preferred_element_type=jnp.float32) / sums).astype(jnp.bfloat16))
        return mixed

    def store_mixed(pair, mixed):
        for i in range(2):
            mix_v[:, pl.ds(pl.multiple_of(pair * COLS + i * head_dim, head_dim), head_dim)] = mixed[i]

    def refill(pair):
        for which in range(3):
            start_unit(3 * pair + which + n_slots, (which + n_slots) % 3)

    def wait_pair(pair):
        for which in range(3):
            wait_unit(3 * pair + which)

    wait_pair(0)
    project(0)
    refill(0)

    def pair_step(pair, carry):
        wait_pair(pair)
        mixed = attend(pair - 1)
        project(pair)
        store_mixed(pair - 1, mixed)
        refill(pair)
        return carry

    lax.fori_loop(1, pairs, pair_step, 0)
    store_mixed(pairs - 1, attend(pairs - 1))

    def store_z(n):
        return pltpu.make_async_copy(z_v.at[n % 2], z_out.at[:, pl.ds(pl.multiple_of(n * COLS, COLS), COLS)], z_sem.at[n % 2])

    def out_step(n, carry):
        wait_unit(3 * pairs + n)
        product = jnp.dot(mix_v[...], weight(3 * pairs + n), preferred_element_type=jnp.float32).astype(jnp.bfloat16)

        @pl.when(n >= 2)
        def _():
            store_z(n - 2).wait()

        z_v[n % 2] = (y_v[n].astype(jnp.float32) + product.astype(jnp.float32)).astype(jnp.bfloat16)
        store_z(n).start()
        start_unit(3 * pairs + n + n_slots, 0)
        return carry

    lax.fori_loop(0, depth, out_step, 0)
    store_z(depth - 2).wait()
    store_z(depth - 1).wait()
    for step in range(1, ep):
        meta_copy(step).wait_send()
    for j in range(blocks):
        swap_rows(j).wait_send()
    swap_resid.wait_send()
    for j in range(blocks - 2, blocks):
        for kind in range(6):
            ring_copy(kind, j).wait_send()
        for side in range(2):
            y_copy(side, j).wait_send()


def combine_and_attend(ep, pp, expert_out, expert_ids, slot_ids, gate_vals, residual, norm_scale, w_query, w_key, w_value, w_out):
    experts, cap, width = expert_out.shape
    tokens, top = expert_ids.shape
    heads, head_dim = w_query.shape[1:]
    sizes = (ep, pp, experts, cap, width, tokens, top, heads, head_dim)
    blocks = width // 2 // COLS
    depth = width // COLS
    chip_rows = 2 * experts * cap // ep
    any_spec = pl.BlockSpec(memory_space=pl.ANY)
    vmem_spec = pl.BlockSpec(memory_space=pltpu.VMEM)
    dma = pltpu.SemaphoreType.DMA

    def by_head(weights):
        return jnp.swapaxes(weights, 0, 1).reshape(heads, depth, COLS, head_dim)

    return pl.pallas_call(
        functools.partial(layer_kernel, sizes),
        out_shape=jax.ShapeDtypeStruct((tokens, width), jnp.bfloat16),
        in_specs=[any_spec, vmem_spec, vmem_spec, vmem_spec, any_spec, vmem_spec] + [any_spec] * 4,
        out_specs=any_spec,
        scratch_shapes=[
            pltpu.VMEM((SLOTS, 2 * experts, cap, COLS), jnp.bfloat16),
            pltpu.VMEM((2, tokens, width // 2), jnp.bfloat16),
            pltpu.VMEM((ep, 2 * top, tokens), jnp.float32),
            pltpu.VMEM((8, 3 * tokens, chip_rows), jnp.bfloat16),
            pltpu.VMEM((6, 2, tokens, COLS), jnp.float32),
            pltpu.VMEM((6, blocks, tokens, COLS), jnp.float32),
            pltpu.VMEM((2, 2, tokens, COLS), jnp.bfloat16),
            pltpu.VMEM((2 * blocks, tokens, COLS), jnp.bfloat16),
            pltpu.VMEM((tokens, COLS), jnp.float32),
            pltpu.VMEM((tokens, width), jnp.bfloat16),
            pltpu.VMEM((2, 3, tokens, COLS), jnp.bfloat16),
            pltpu.VMEM((tokens, heads * head_dim), jnp.bfloat16),
            pltpu.VMEM((2, tokens, COLS), jnp.bfloat16),
            dma((blocks,)), dma((blocks,)), dma((blocks,)), dma, dma, dma, dma((ep - 1,)), dma((ep - 1,)),
            dma((6, blocks)), dma((6, blocks)), dma((2, blocks)), dma((2 * blocks,)), dma((SLOTS, 2)), dma((2,)),
        ],
        compiler_params=pltpu.CompilerParams(collective_id=0, has_side_effects=True, vmem_limit_bytes=67043328),
    )(expert_out, expert_ids.T, slot_ids.T, gate_vals.T, residual, norm_scale[None],
      by_head(w_query), by_head(w_key), by_head(w_value), w_out.reshape(heads * head_dim // COLS, COLS, width))


def solution(mesh):
    ep_size = mesh.shape['ep']
    pp_size = mesh.shape['pp']
    token_spec = P(('data', 'pp'), 'ep', None, None)
    weight_spec = P('pp', None, None, None)

    def body(expert_out, expert_ids, slot_ids, gate_vals, residual, norm_scale, w_query, w_key, w_value, w_out):
        result = combine_and_attend(
            ep_size, pp_size, expert_out[0], expert_ids[0, 0], slot_ids[0, 0], gate_vals[0, 0], residual[0, 0],
            norm_scale[0], w_query[0], w_key[0], w_value[0], w_out[0])
        return result[None, None]

    return jax.shard_map(body, mesh=mesh, in_specs=(token_spec, token_spec, token_spec, token_spec, token_spec, P('pp', None), weight_spec, weight_spec, weight_spec, weight_spec), out_specs=token_spec, check_vma=False)
```

```python
import functools

import jax
import jax.numpy as jnp
from jax import lax
from jax.experimental import pallas as pl
from jax.experimental.pallas import tpu as pltpu
from jax.sharding import PartitionSpec as P

NORM_EPS = 1e-6
COLS = 256
CHUNK = 96
RING_SLOTS = 10
MESH = pl.DeviceIdType.MESH


def layer_kernel(sizes, o_hbm, ids, slots, gates, h_hbm, scale_ref, wq_hbm, wk_hbm, wv_hbm, wo_hbm, z_out,
                 pool, resid_v, meta, gate_mats, send_v, recv_v, ysend_v, y_v, square_v, x_v, q_v, kv_v, mix_v, z_v,
                 rows_loc, rows_ss, rows_rs, res_loc, res_ss, res_rs, meta_ss, meta_rs,
                 ring_ss, ring_rs, y_ss, y_rs, relay_ss, relay_rs, mix_ss, mix_rs, w_sem, z_sem, zr_ss, zr_rs):
    ep, pp, experts, cap, width, tokens, top, heads, head_dim = sizes
    chips = ep // 2
    half = width // 2
    blocks = half // COLS
    chunks = tokens // CHUNK
    steps = chunks * blocks
    depth = width // COLS
    pairs = heads // 4
    cap_dev = cap // ep
    chip_rows = 2 * experts * cap_dev
    units = chunks * pairs * 3
    me = lax.axis_index('ep')
    stage = lax.axis_index('pp')
    chip, core = me // 2, me % 2
    partner = chip * 2 + (1 - core)
    ahead, behind, across = (chip + 1) % chips, (chip + chips - 1) % chips, (chip + 2) % chips
    next_stage, prev_stage = (stage + 1) % pp, (stage + pp - 1) % pp
    right, left = 2 * ahead + core, 2 * behind + core
    owners = (2 * across, 2 * across + 1, 2 * ahead + 1, 2 * behind, 2 * ahead, 2 * behind + 1, 2 * chip, 2 * chip + 1)

    def span(t):
        return pl.ds(pl.multiple_of(t * CHUNK, CHUNK), CHUNK)

    def lanes_at(start, size=COLS):
        return pl.ds(pl.multiple_of(start, 128), size)

    def local_rows(j):
        return pltpu.make_async_copy(o_hbm.at[:, :, lanes_at(core * half + j * COLS)],
                                     pool.at[j, pl.ds(core * experts, experts)], rows_loc.at[j])

    def swap_rows(j):
        return pltpu.make_async_remote_copy(
            src_ref=o_hbm.at[:, :, lanes_at((1 - core) * half + j * COLS)], dst_ref=pool.at[j, pl.ds(core * experts, experts)],
            send_sem=rows_ss.at[j], recv_sem=rows_rs.at[j], device_id={'ep': partner}, device_id_type=MESH)

    local_resid = pltpu.make_async_copy(h_hbm.at[:, lanes_at(core * half, half)], resid_v.at[core], res_loc)
    swap_resid = pltpu.make_async_remote_copy(
        src_ref=h_hbm.at[:, lanes_at((1 - core) * half, half)], dst_ref=resid_v.at[core],
        send_sem=res_ss, recv_sem=res_rs, device_id={'ep': partner}, device_id_type=MESH)

    def meta_copy(step):
        return pltpu.make_async_remote_copy(
            src_ref=meta.at[me], dst_ref=meta.at[me], send_sem=meta_ss.at[step - 1], recv_sem=meta_rs.at[step - 1],
            device_id={'ep': (me + step) % ep}, device_id_type=MESH)

    def ring_copy(kind, s):
        target = right if kind % 2 == 0 else left
        return pltpu.make_async_remote_copy(
            src_ref=send_v.at[kind, s % 2], dst_ref=recv_v.at[kind, s], send_sem=ring_ss.at[kind, s],
            recv_sem=ring_rs.at[kind, s], device_id={'ep': target}, device_id_type=MESH)

    def y_copy(side, s):
        return pltpu.make_async_remote_copy(
            src_ref=ysend_v.at[side, s % 2], dst_ref=y_v.at[side, core * blocks + s % blocks, span(s // blocks)],
            send_sem=y_ss.at[side, s], recv_sem=y_rs.at[core, s],
            device_id={'pp': next_stage, 'ep': 2 * chip + side}, device_id_type=MESH)

    def y_relay(part, s):
        piece = y_v.at[core, part * blocks + s % blocks, span(s // blocks)]
        return pltpu.make_async_remote_copy(
            src_ref=piece, dst_ref=piece, send_sem=relay_ss.at[part, s], recv_sem=relay_rs.at[part, s],
            device_id={'ep': partner}, device_id_type=MESH)

    def mix_copy(pair, t):
        block = mix_v.at[core * pairs + pair, :, span(t)]
        return pltpu.make_async_remote_copy(
            src_ref=block, dst_ref=block, send_sem=mix_ss.at[t, pair], recv_sem=mix_rs.at[t, pair],
            device_id={'ep': partner}, device_id_type=MESH)

    def qkv_copies(which, pair, slot):
        w_hbm = (wq_hbm, wk_hbm, wv_hbm)[which]
        return [pltpu.make_async_copy(w_hbm.at[2 * (core * pairs + pair) + i],
                                      pool.at[slot, 0:depth, :, i * head_dim:(i + 1) * head_dim], w_sem.at[slot, i]) for i in range(2)]

    def out_copies(n):
        mid = depth // 2
        return [pltpu.make_async_copy(wo_hbm.at[i * mid:(i + 1) * mid, :, lanes_at(core * half + n * COLS)],
                                      pool.at[n, i * mid:(i + 1) * mid], w_sem.at[n, i]) for i in range(2)]

    def slot_of(unit):
        return blocks + unit % RING_SLOTS

    def start_all(copies):
        for copy in copies:
            copy.start()

    def wait_all(copies):
        for copy in copies:
            copy.wait()

    for j in range(blocks):
        local_rows(j).start()
    local_resid.start()
    kv_v[...] = jnp.zeros_like(kv_v)
    row_ids = jnp.where(slots[...] >= 0, ids[...] * cap_dev + slots[...] - me * cap_dev, -1)
    meta[me, 0:top, :] = row_ids.astype(jnp.float32)
    meta[me, top:2 * top, :] = gates[...]

    barrier = pltpu.get_barrier_semaphore()
    for step in range(1, ep):
        pl.semaphore_signal(barrier, inc=1, device_id={'ep': (me + step) % ep}, device_id_type=MESH)
    for side in range(2):
        pl.semaphore_signal(barrier, inc=1, device_id={'pp': next_stage, 'ep': 2 * chip + side}, device_id_type=MESH)
        pl.semaphore_signal(barrier, inc=1, device_id={'pp': prev_stage, 'ep': 2 * chip + side}, device_id_type=MESH)
    pl.semaphore_wait(barrier, ep - 1 + 4)

    for step in range(1, ep):
        meta_copy(step).start()
    for j in range(blocks):
        swap_rows(j).start()
    swap_resid.start()

    def build_gates(role):
        table = jnp.transpose(meta[owners[role]])
        wanted = (lax.broadcasted_iota(jnp.int32, (tokens, chip_rows), 1) + chip * chip_rows).astype(jnp.float32)
        total = jnp.zeros((tokens, chip_rows), jnp.float32)
        for t in range(top):
            total = total + jnp.where(table[:, t:t + 1] == wanted, table[:, top + t:top + t + 1], 0.0)
        high = total.astype(jnp.bfloat16)
        rest = total - high.astype(jnp.float32)
        mid = rest.astype(jnp.bfloat16)
        low = (rest - mid.astype(jnp.float32)).astype(jnp.bfloat16)
        for t in range(chunks):
            for i, term in enumerate((high, mid, low)):
                gate_mats[role, t, i * CHUNK:(i + 1) * CHUNK] = term[t * CHUNK:(t + 1) * CHUNK]

    def contribution(role, s):
        slot0 = pl.multiple_of(owners[role] * cap_dev, cap_dev)
        rows = pool[s % blocks, :, pl.ds(slot0, cap_dev), :].reshape(chip_rows, COLS)
        parts = jnp.dot(gate_mats[role, s // blocks], rows, preferred_element_type=jnp.float32)
        return parts[2 * CHUNK:] + parts[CHUNK:2 * CHUNK] + parts[:CHUNK]

    def leaf(kind, s):
        @pl.when(s >= 2)
        def _():
            ring_copy(kind, s - 2).wait_send()

        send_v[kind, s % 2] = contribution(kind, s)
        ring_copy(kind, s).start()

    def forward(kind, s):
        own = contribution(kind, s)

        @pl.when(s >= 2)
        def _():
            ring_copy(kind, s - 2).wait_send()

        ring_copy(kind - 4, s).wait_recv()
        send_v[kind, s % 2] = own + recv_v[kind - 4, s]
        ring_copy(kind, s).start()

    def finish(side, s):
        near, far = ((3, 4), (2, 5))[side]
        own = contribution(6 + side, s)

        @pl.when(s >= 2)
        def _():
            y_copy(side, s - 2).wait_send()

        ring_copy(near, s).wait_recv()
        ring_copy(far, s).wait_recv()
        resid = resid_v[side, span(s // blocks), lanes_at(s % blocks * COLS)].astype(jnp.float32)
        ysend_v[side, s % 2] = (resid + (own + recv_v[near, s] + recv_v[far, s])).astype(jnp.bfloat16)
        y_copy(side, s).start()

    def pass_on(s):
        for part in range(2):
            pltpu.make_async_copy(ysend_v.at[0, 0], ysend_v.at[0, 0], y_rs.at[part, s]).wait()
            y_relay(part, s).start()

    def take(s):
        @pl.when(s % blocks == 0)
        def _():
            square_v[...] = jnp.zeros_like(square_v)

        for part in range(2):
            y_relay(part, s).wait_recv()
            for seq in range(2):
                piece = y_v[seq, part * blocks + s % blocks, span(s // blocks)].astype(jnp.float32)
                square_v[seq] += piece * piece

    def normalize(t):
        for seq in range(2):
            mean = jnp.sum(square_v[seq], axis=-1, keepdims=True) / width
            inv_rms = lax.rsqrt(mean + NORM_EPS)
            for i in range(depth):
                cols = slice(i * COLS, (i + 1) * COLS)
                x_v[seq * CHUNK:(seq + 1) * CHUNK, cols] = (
                    y_v[seq, i, span(t)].astype(jnp.float32) * inv_rms * scale_ref[:, cols]).astype(jnp.bfloat16)

    def unit_of(which, pair, t):
        return (t * pairs + pair) * 3 + which

    def wait_pair(pair, t):
        for which in range(3):
            wait_all(qkv_copies(which, 0, slot_of(unit_of(which, pair, t))))

    def refill(pair, t):
        for which in range(3):
            unit = unit_of(which, pair, t) + RING_SLOTS

            @pl.when(unit < units)
            def _():
                start_all(qkv_copies((which + RING_SLOTS) % 3, unit // 3 % pairs, slot_of(unit)))

    def project(pair, t):
        for which in range(3):
            weight = pool[slot_of(unit_of(which, pair, t)), 0:depth].reshape(width, COLS)
            product = jnp.dot(x_v[...], weight, preferred_element_type=jnp.float32).astype(jnp.bfloat16)
            if which == 0:
                q_v[pair % 2] = product
            else:
                for seq in range(2):
                    kv_v[which - 1, pair, seq, span(t)] = product[seq * CHUNK:(seq + 1) * CHUNK]

    def attend(pair, t):
        causal = (lax.broadcasted_iota(jnp.int32, (CHUNK, tokens), 0) + t * CHUNK
                  >= lax.broadcasted_iota(jnp.int32, (CHUNK, tokens), 1))
        mixed = []
        for seq in range(2):
            for i in range(2):
                lanes = slice(i * head_dim, (i + 1) * head_dim)
                q = q_v[pair % 2, seq * CHUNK:(seq + 1) * CHUNK, lanes]
                k, v = kv_v[0, pair, seq, :, lanes], kv_v[1, pair, seq, :, lanes]
                scores = lax.dot_general(q, k, (((1,), (1,)), ((), ())), preferred_element_type=jnp.float32) * head_dim ** -0.5
                scores = jnp.where(causal, scores, -1e30)
                exps = jnp.exp(scores - jnp.max(scores, axis=-1, keepdims=True))
                sums = jnp.sum(exps, axis=-1, keepdims=True)
                mixed.append((jnp.dot(exps.astype(jnp.bfloat16), v, preferred_element_type=jnp.float32) / sums).astype(jnp.bfloat16))
        return mixed

    def store_mixed(pair, t, mixed):
        for seq in range(2):
            for i in range(2):
                mix_v[core * pairs + pair, seq, span(t), i * head_dim:(i + 1) * head_dim] = mixed[2 * seq + i]
        mix_copy(pair, t).start()

    for step in range(1, ep):
        meta_copy(step).wait_recv()

    def ring_step(s, carry):
        @pl.when(s < steps)
        def _():
            @pl.when(s < blocks)
            def _():
                local_rows(s).wait()
                swap_rows(s).wait_recv()

            for kind in range(4):
                @pl.when(s == 0)
                def _():
                    build_gates(kind)

                leaf(kind, s)

        @pl.when(s == 0)
        def _():
            for role in range(4, 8):
                build_gates(role)
            local_resid.wait()
            swap_resid.wait_recv()
            for unit in range(RING_SLOTS):
                start_all(qkv_copies(unit % 3, unit // 3, slot_of(unit)))

        @pl.when(jnp.logical_and(s >= 1, s < steps + 1))
        def _():
            forward(4, s - 1)
            forward(5, s - 1)

        @pl.when(jnp.logical_and(s >= 2, s < steps + 2))
        def _():
            finish(0, s - 2)
            finish(1, s - 2)

            @pl.when(s - 2 >= steps - blocks)
            def _():
                start_all(out_copies(s - 2 - (steps - blocks)))

        @pl.when(jnp.logical_and(s >= 3, s < steps + 3))
        def _():
            pass_on(s - 3)

        @pl.when(s >= 4)
        def _():
            take(s - 4)

        lag = s % blocks - 3

        @pl.when(jnp.logical_and(s >= blocks, lag == 0))
        def _():
            normalize(s // blocks - 1)

        @pl.when(jnp.logical_and(jnp.logical_and(s >= blocks, s < steps), lag >= 0))
        def _():
            def one_pair(pair, carry):
                t = s // blocks - 1
                wait_pair(pair, t)
                project(pair, t)
                store_mixed(pair, t, attend(pair, t))
                refill(pair, t)
                return carry

            lax.fori_loop(2 * lag, jnp.minimum(2 * lag + 2, pairs), one_pair, 0)
        return carry

    lax.fori_loop(0, steps + 4, ring_step, 0)

    last = chunks - 1
    wait_pair(0, last)
    project(0, last)
    refill(0, last)

    def pair_step(pair, carry):
        wait_pair(pair, last)
        mixed = attend(pair - 1, last)
        project(pair, last)
        store_mixed(pair - 1, last, mixed)
        refill(pair, last)
        return carry

    lax.fori_loop(1, pairs, pair_step, 0)
    store_mixed(pairs - 1, last, attend(pairs - 1, last))

    for t in range(chunks):
        for pair in range(pairs):
            mix_copy(pair, t).wait_recv()

    def store_z(n):
        return pltpu.make_async_copy(z_v.at[n % 2, core], z_out.at[:, lanes_at(core * half + n * COLS)], z_sem.at[n])

    def send_z(n):
        return pltpu.make_async_remote_copy(
            src_ref=z_v.at[n % 2, 1 - core], dst_ref=z_out.at[:, lanes_at(core * half + n * COLS)],
            send_sem=zr_ss.at[n], recv_sem=zr_rs.at[n], device_id={'ep': partner}, device_id_type=MESH)

    def out_step(n, carry):
        wait_all(out_copies(n))
        mixed = jnp.concatenate([mix_v[i].reshape(2 * tokens, COLS) for i in range(depth)], axis=1)
        weight = pool[n, 0:depth].reshape(width, COLS)
        product = jnp.dot(mixed, weight, preferred_element_type=jnp.float32).astype(jnp.bfloat16)

        @pl.when(n >= 2)
        def _():
            store_z(n - 2).wait()
            send_z(n - 2).wait_send()

        for seq in range(2):
            resid = y_v[seq, core * blocks + n].astype(jnp.float32)
            z_v[n % 2, seq] = (resid + product[seq * tokens:(seq + 1) * tokens].astype(jnp.float32)).astype(jnp.bfloat16)
        send_z(n).start()
        store_z(n).start()
        return carry

    lax.fori_loop(0, blocks, out_step, 0)
    for n in range(blocks - 2, blocks):
        store_z(n).wait()
        send_z(n).wait_send()
    for n in range(blocks):
        send_z(n).wait_recv()
    for step in range(1, ep):
        meta_copy(step).wait_send()
    for j in range(blocks):
        swap_rows(j).wait_send()
    swap_resid.wait_send()
    for t in range(chunks):
        for pair in range(pairs):
            mix_copy(pair, t).wait_send()
    for s in range(steps):
        for part in range(2):
            y_relay(part, s).wait_send()
    for s in range(steps - 2, steps):
        for kind in range(6):
            ring_copy(kind, s).wait_send()
        for side in range(2):
            y_copy(side, s).wait_send()


def combine_and_attend(ep, pp, expert_out, expert_ids, slot_ids, gate_vals, residual, norm_scale, w_query, w_key, w_value, w_out):
    experts, cap, width = expert_out.shape
    tokens, top = expert_ids.shape
    heads, head_dim = w_query.shape[1:]
    sizes = (ep, pp, experts, cap, width, tokens, top, heads, head_dim)
    half = width // 2
    blocks = half // COLS
    chunks = tokens // CHUNK
    steps = chunks * blocks
    depth = width // COLS
    pairs = heads // 4
    chip_rows = 2 * experts * cap // ep
    any_spec = pl.BlockSpec(memory_space=pl.ANY)
    vmem_spec = pl.BlockSpec(memory_space=pltpu.VMEM)
    dma = pltpu.SemaphoreType.DMA

    def by_head(weights):
        return jnp.swapaxes(weights, 0, 1).reshape(heads, depth, COLS, head_dim)

    return pl.pallas_call(
        functools.partial(layer_kernel, sizes),
        out_shape=jax.ShapeDtypeStruct((tokens, width), jnp.bfloat16),
        in_specs=[any_spec, vmem_spec, vmem_spec, vmem_spec, any_spec, vmem_spec] + [any_spec] * 4,
        out_specs=any_spec,
        scratch_shapes=[
            pltpu.VMEM((blocks + RING_SLOTS, 2 * experts, cap, COLS), jnp.bfloat16),
            pltpu.VMEM((2, tokens, half), jnp.bfloat16),
            pltpu.VMEM((ep, 2 * top, tokens), jnp.float32),
            pltpu.VMEM((8, chunks, 3 * CHUNK, chip_rows), jnp.bfloat16),
            pltpu.VMEM((6, 2, CHUNK, COLS), jnp.float32),
            pltpu.VMEM((6, steps, CHUNK, COLS), jnp.float32),
            pltpu.VMEM((2, 2, CHUNK, COLS), jnp.bfloat16),
            pltpu.VMEM((2, depth, tokens, COLS), jnp.bfloat16),
            pltpu.VMEM((2, CHUNK, COLS), jnp.float32),
            pltpu.VMEM((2 * CHUNK, width), jnp.bfloat16),
            pltpu.VMEM((2, 2 * CHUNK, COLS), jnp.bfloat16),
            pltpu.VMEM((2, pairs, 2, tokens, COLS), jnp.bfloat16),
            pltpu.VMEM((2 * pairs, 2, tokens, COLS), jnp.bfloat16),
            pltpu.VMEM((2, 2, tokens, COLS), jnp.bfloat16),
            dma((blocks,)), dma((blocks,)), dma((blocks,)), dma, dma, dma, dma((ep - 1,)), dma((ep - 1,)),
            dma((6, steps)), dma((6, steps)), dma((2, steps)), dma((2, steps)), dma((2, steps)), dma((2, steps)),
            dma((chunks, pairs)), dma((chunks, pairs)), dma((blocks + RING_SLOTS, 2)), dma((blocks,)), dma((blocks,)), dma((blocks,)),
        ],
        compiler_params=pltpu.CompilerParams(collective_id=0, has_side_effects=True, vmem_limit_bytes=67043328),
    )(expert_out, expert_ids.T, slot_ids.T, gate_vals.T, residual, norm_scale[None],
      by_head(w_query), by_head(w_key), by_head(w_value), w_out.reshape(depth, COLS, width))


def solution(mesh):
    ep_size = mesh.shape['ep']
    pp_size = mesh.shape['pp']
    token_spec = P(('data', 'pp'), 'ep', None, None)
    weight_spec = P('pp', None, None, None)

    def body(expert_out, expert_ids, slot_ids, gate_vals, residual, norm_scale, w_query, w_key, w_value, w_out):
        result = combine_and_attend(
            ep_size, pp_size, expert_out[0], expert_ids[0, 0], slot_ids[0, 0], gate_vals[0, 0], residual[0, 0],
            norm_scale[0], w_query[0], w_key[0], w_value[0], w_out[0])
        return result[None, None]

    return jax.shard_map(body, mesh=mesh, in_specs=(token_spec, token_spec, token_spec, token_spec, token_spec, P('pp', None), weight_spec, weight_spec, weight_spec, weight_spec), out_specs=token_spec, check_vma=False)
```

```python
import functools

import jax
import jax.numpy as jnp
from jax import lax
from jax.experimental import pallas as pl
from jax.experimental.pallas import tpu as pltpu
from jax.sharding import PartitionSpec as P

NORM_EPS = 1e-6
COLS = 256
CHUNK = 96
RING_PAIRS = 3
MESH = pl.DeviceIdType.MESH


def layer_kernel(sizes, o_hbm, ids, slots, gates, h_hbm, scale_ref, wq_hbm, wk_hbm, wv_hbm, wo_hbm, z_out,
                 pool, resid_v, meta, gate_mats, send_v, recv_v, ysend_v, y_v, square_v, x_v, q_v, kv_v, mix_v, z_v,
                 rows_loc, rows_ss, rows_rs, res_loc, res_ss, res_rs, meta_ss, meta_rs,
                 ring_ss, ring_rs, y_ss, y_rs, relay_ss, relay_rs, mix_ss, mix_rs, w_sem, z_sem, zr_ss, zr_rs):
    ep, pp, experts, cap, width, tokens, top, heads, head_dim = sizes
    chips = ep // 2
    half = width // 2
    blocks = half // COLS
    chunks = tokens // CHUNK
    steps = chunks * blocks
    depth = width // COLS
    pairs = heads // 4
    cap_dev = cap // ep
    chip_rows = 2 * experts * cap_dev
    me = lax.axis_index('ep')
    stage = lax.axis_index('pp')
    chip, core = me // 2, me % 2
    partner = chip * 2 + (1 - core)
    ahead, behind, across = (chip + 1) % chips, (chip + chips - 1) % chips, (chip + 2) % chips
    next_stage, prev_stage = (stage + 1) % pp, (stage + pp - 1) % pp
    right, left = 2 * ahead + core, 2 * behind + core
    owners = (2 * across, 2 * across + 1, 2 * ahead + 1, 2 * behind, 2 * ahead, 2 * behind + 1, 2 * chip, 2 * chip + 1)

    def span(t):
        return pl.ds(pl.multiple_of(t * CHUNK, CHUNK), CHUNK)

    def lanes_at(start, size=COLS):
        return pl.ds(pl.multiple_of(start, 128), size)

    def local_rows(j):
        return pltpu.make_async_copy(o_hbm.at[:, :, lanes_at(core * half + j * COLS)],
                                     pool.at[j, pl.ds(core * experts, experts)], rows_loc.at[j])

    def swap_rows(j):
        return pltpu.make_async_remote_copy(
            src_ref=o_hbm.at[:, :, lanes_at((1 - core) * half + j * COLS)], dst_ref=pool.at[j, pl.ds(core * experts, experts)],
            send_sem=rows_ss.at[j], recv_sem=rows_rs.at[j], device_id={'ep': partner}, device_id_type=MESH)

    local_resid = pltpu.make_async_copy(h_hbm.at[:, lanes_at(core * half, half)], resid_v.at[core], res_loc)
    swap_resid = pltpu.make_async_remote_copy(
        src_ref=h_hbm.at[:, lanes_at((1 - core) * half, half)], dst_ref=resid_v.at[core],
        send_sem=res_ss, recv_sem=res_rs, device_id={'ep': partner}, device_id_type=MESH)

    def meta_copy(step):
        return pltpu.make_async_remote_copy(
            src_ref=meta.at[me], dst_ref=meta.at[me], send_sem=meta_ss.at[step - 1], recv_sem=meta_rs.at[step - 1],
            device_id={'ep': (me + step) % ep}, device_id_type=MESH)

    def ring_copy(kind, s):
        target = right if kind % 2 == 0 else left
        return pltpu.make_async_remote_copy(
            src_ref=send_v.at[kind, s % 2], dst_ref=recv_v.at[kind, s], send_sem=ring_ss.at[kind, s],
            recv_sem=ring_rs.at[kind, s], device_id={'ep': target}, device_id_type=MESH)

    def y_copy(side, s):
        return pltpu.make_async_remote_copy(
            src_ref=ysend_v.at[side, s % 2], dst_ref=y_v.at[side, core * blocks + s % blocks, span(s // blocks)],
            send_sem=y_ss.at[side, s], recv_sem=y_rs.at[core, s],
            device_id={'pp': next_stage, 'ep': 2 * chip + side}, device_id_type=MESH)

    def y_relay(part, s):
        piece = y_v.at[core, part * blocks + s % blocks, span(s // blocks)]
        return pltpu.make_async_remote_copy(
            src_ref=piece, dst_ref=piece, send_sem=relay_ss.at[part, s], recv_sem=relay_rs.at[part, s],
            device_id={'ep': partner}, device_id_type=MESH)

    def mix_copy(pair, t):
        block = mix_v.at[core * pairs + pair, :, span(t)]
        return pltpu.make_async_remote_copy(
            src_ref=block, dst_ref=block, send_sem=mix_ss.at[t, pair], recv_sem=mix_rs.at[t, pair],
            device_id={'ep': partner}, device_id_type=MESH)

    def qkv_copies(which, pair, slot):
        w_hbm = (wq_hbm, wk_hbm, wv_hbm)[which]
        return [pltpu.make_async_copy(w_hbm.at[2 * (core * pairs + pair) + i],
                                      pool.at[slot, 0:depth, :, i * head_dim:(i + 1) * head_dim], w_sem.at[slot, i]) for i in range(2)]

    def out_copies(n):
        mid = depth // 2
        return [pltpu.make_async_copy(wo_hbm.at[i * mid:(i + 1) * mid, :, lanes_at(core * half + n * COLS)],
                                      pool.at[n, i * mid:(i + 1) * mid], w_sem.at[n, i]) for i in range(2)]

    def slot_of(which, pair):
        return blocks + pair % RING_PAIRS * 3 + which

    def start_all(copies):
        for copy in copies:
            copy.start()

    def wait_all(copies):
        for copy in copies:
            copy.wait()

    for j in range(blocks):
        local_rows(j).start()
    local_resid.start()
    row_ids = jnp.where(slots[...] >= 0, ids[...] * cap_dev + slots[...] - me * cap_dev, -1)
    meta[me, 0:top, :] = row_ids.astype(jnp.float32)
    meta[me, top:2 * top, :] = gates[...]

    barrier = pltpu.get_barrier_semaphore()
    for step in range(1, ep):
        pl.semaphore_signal(barrier, inc=1, device_id={'ep': (me + step) % ep}, device_id_type=MESH)
    for side in range(2):
        pl.semaphore_signal(barrier, inc=1, device_id={'pp': next_stage, 'ep': 2 * chip + side}, device_id_type=MESH)
        pl.semaphore_signal(barrier, inc=1, device_id={'pp': prev_stage, 'ep': 2 * chip + side}, device_id_type=MESH)
    pl.semaphore_wait(barrier, ep - 1 + 4)

    for step in range(1, ep):
        meta_copy(step).start()
    for j in range(blocks):
        swap_rows(j).start()
    swap_resid.start()

    def build_gates(role):
        table = jnp.transpose(meta[owners[role]])
        wanted = (lax.broadcasted_iota(jnp.int32, (tokens, chip_rows), 1) + chip * chip_rows).astype(jnp.float32)
        total = jnp.zeros((tokens, chip_rows), jnp.float32)
        for t in range(top):
            total = total + jnp.where(table[:, t:t + 1] == wanted, table[:, top + t:top + t + 1], 0.0)
        high = total.astype(jnp.bfloat16)
        rest = total - high.astype(jnp.float32)
        mid = rest.astype(jnp.bfloat16)
        low = (rest - mid.astype(jnp.float32)).astype(jnp.bfloat16)
        for t in range(chunks):
            for i, term in enumerate((high, mid, low)):
                gate_mats[role, t, i * CHUNK:(i + 1) * CHUNK] = term[t * CHUNK:(t + 1) * CHUNK]

    def contribution(role, s):
        slot0 = pl.multiple_of(owners[role] * cap_dev, cap_dev)
        rows = pool[s % blocks, :, pl.ds(slot0, cap_dev), :].reshape(chip_rows, COLS)
        parts = jnp.dot(gate_mats[role, s // blocks], rows, preferred_element_type=jnp.float32)
        return parts[2 * CHUNK:] + parts[CHUNK:2 * CHUNK] + parts[:CHUNK]

    def leaf(kind, s):
        @pl.when(s >= 2)
        def _():
            ring_copy(kind, s - 2).wait_send()

        send_v[kind, s % 2] = contribution(kind, s)
        ring_copy(kind, s).start()

    def forward(kind, s):
        own = contribution(kind, s)

        @pl.when(s >= 2)
        def _():
            ring_copy(kind, s - 2).wait_send()

        ring_copy(kind - 4, s).wait_recv()
        send_v[kind, s % 2] = own + recv_v[kind - 4, s]
        ring_copy(kind, s).start()

    def finish(side, s):
        near, far = ((3, 4), (2, 5))[side]
        own = contribution(6 + side, s)

        @pl.when(s >= 2)
        def _():
            y_copy(side, s - 2).wait_send()

        ring_copy(near, s).wait_recv()
        ring_copy(far, s).wait_recv()
        resid = resid_v[side, span(s // blocks), lanes_at(s % blocks * COLS)].astype(jnp.float32)
        ysend_v[side, s % 2] = (resid + (own + recv_v[near, s] + recv_v[far, s])).astype(jnp.bfloat16)
        y_copy(side, s).start()

    def pass_on(s):
        for part in range(2):
            pltpu.make_async_copy(ysend_v.at[0, 0], ysend_v.at[0, 0], y_rs.at[part, s]).wait()
            y_relay(part, s).start()

    def take(s):
        @pl.when(s % blocks == 0)
        def _():
            square_v[...] = jnp.zeros_like(square_v)

        for part in range(2):
            y_relay(part, s).wait_recv()
            for seq in range(2):
                piece = y_v[seq, part * blocks + s % blocks, span(s // blocks)].astype(jnp.float32)
                square_v[seq] += piece * piece

    def normalize(t):
        for seq in range(2):
            mean = jnp.sum(square_v[seq], axis=-1, keepdims=True) / width
            inv_rms = lax.rsqrt(mean + NORM_EPS)
            for i in range(depth):
                cols = slice(i * COLS, (i + 1) * COLS)
                x_v[seq * CHUNK:(seq + 1) * CHUNK, cols] = (
                    y_v[seq, i, span(t)].astype(jnp.float32) * inv_rms * scale_ref[:, cols]).astype(jnp.bfloat16)

    def fetch(pair):
        for which in range(3):
            start_all(qkv_copies(which, pair, slot_of(which, pair)))

    def wait_pair(i, pair, t):
        @pl.when(jnp.logical_or(t == 0, i >= RING_PAIRS))
        def _():
            for which in range(3):
                wait_all(qkv_copies(which, 0, slot_of(which, pair)))

    def refill(pair, t):
        odd = t % 2
        later = pair + (1 - 2 * odd) * RING_PAIRS

        @pl.when(jnp.logical_and(later >= 0, later < pairs))
        def _():
            fetch(later)

    def project(pair, t):
        for which in range(3):
            weight = pool[slot_of(which, pair), 0:depth].reshape(width, COLS)
            product = jnp.dot(x_v[...], weight, preferred_element_type=jnp.float32).astype(jnp.bfloat16)
            if which == 0:
                q_v[pair % 2] = product
            else:
                for seq in range(2):
                    kv_v[which - 1, pair, seq, span(t)] = product[seq * CHUNK:(seq + 1) * CHUNK]

    def attend(pair, t):
        causal = (lax.broadcasted_iota(jnp.int32, (CHUNK, tokens), 0) + t * CHUNK
                  >= lax.broadcasted_iota(jnp.int32, (CHUNK, tokens), 1))
        mixed = []
        for seq in range(2):
            for i in range(2):
                lanes = slice(i * head_dim, (i + 1) * head_dim)
                q = q_v[pair % 2, seq * CHUNK:(seq + 1) * CHUNK, lanes]
                k, v = kv_v[0, pair, seq, :, lanes], kv_v[1, pair, seq, :, lanes]
                scores = lax.dot_general(q, k, (((1,), (1,)), ((), ())), preferred_element_type=jnp.float32) * head_dim ** -0.5
                scores = jnp.where(causal, scores, -1e30)
                exps = jnp.exp(scores - jnp.max(scores, axis=-1, keepdims=True))
                sums = jnp.sum(exps, axis=-1, keepdims=True)
                mixed.append((jnp.dot(exps.astype(jnp.bfloat16), v, preferred_element_type=jnp.float32) / sums).astype(jnp.bfloat16))
        return mixed

    def store_mixed(pair, t, mixed):
        for seq in range(2):
            for i in range(2):
                mix_v[core * pairs + pair, seq, span(t), i * head_dim:(i + 1) * head_dim] = mixed[2 * seq + i]
        mix_copy(pair, t).start()

    for step in range(1, ep):
        meta_copy(step).wait_recv()

    def ring_step(s, carry):
        @pl.when(s < steps)
        def _():
            @pl.when(s < blocks)
            def _():
                local_rows(s).wait()
                swap_rows(s).wait_recv()

            for kind in range(4):
                @pl.when(s == 0)
                def _():
                    build_gates(kind)

                leaf(kind, s)

        @pl.when(s == 0)
        def _():
            for role in range(4, 8):
                build_gates(role)
            local_resid.wait()
            swap_resid.wait_recv()
            kv_v[...] = jnp.zeros_like(kv_v)

        for which in range(3):
            @pl.when(jnp.logical_and(s % 3 == which, s < 3 * RING_PAIRS))
            def _():
                start_all(qkv_copies(which, s // 3, slot_of(which, s // 3)))

        @pl.when(jnp.logical_and(s >= 1, s < steps + 1))
        def _():
            forward(4, s - 1)
            forward(5, s - 1)

        lag = s % blocks - 4

        @pl.when(jnp.logical_and(jnp.logical_and(s >= blocks, s < steps), lag >= 0))
        def _():
            def one_pair(i, carry):
                t = s // blocks - 1
                odd = t % 2
                pair = odd * (pairs - 1) + (1 - 2 * odd) * i
                wait_pair(i, pair, t)
                project(pair, t)
                refill(pair, t)
                store_mixed(pair, t, attend(pair, t))
                return carry

            lax.fori_loop(3 * lag, jnp.minimum(3 * lag + 3, pairs), one_pair, 0)

        @pl.when(jnp.logical_and(s >= 2, s < steps + 2))
        def _():
            finish(0, s - 2)
            finish(1, s - 2)

            @pl.when(s - 2 >= steps - blocks)
            def _():
                start_all(out_copies(s - 2 - (steps - blocks)))

        @pl.when(jnp.logical_and(s >= 3, s < steps + 3))
        def _():
            pass_on(s - 3)

        @pl.when(s >= 4)
        def _():
            take(s - 4)

        @pl.when(jnp.logical_and(s >= blocks, s % blocks == 3))
        def _():
            normalize(s // blocks - 1)

        return carry

    lax.fori_loop(0, steps + 4, ring_step, 0)

    last = chunks - 1
    flip = last % 2

    def nth(i):
        return pairs - 1 - i if flip else i

    wait_pair(0, nth(0), last)
    project(nth(0), last)
    refill(nth(0), last)

    def pair_step(i, carry):
        wait_pair(i, nth(i), last)
        mixed = attend(nth(i - 1), last)
        project(nth(i), last)
        store_mixed(nth(i - 1), last, mixed)
        refill(nth(i), last)
        return carry

    lax.fori_loop(1, pairs, pair_step, 0)
    store_mixed(nth(pairs - 1), last, attend(nth(pairs - 1), last))

    for t in range(chunks):
        for pair in range(pairs):
            mix_copy(pair, t).wait_recv()

    def store_z(n):
        return pltpu.make_async_copy(z_v.at[n % 2, core], z_out.at[:, lanes_at(core * half + n * COLS)], z_sem.at[n])

    def send_z(n):
        return pltpu.make_async_remote_copy(
            src_ref=z_v.at[n % 2, 1 - core], dst_ref=z_out.at[:, lanes_at(core * half + n * COLS)],
            send_sem=zr_ss.at[n], recv_sem=zr_rs.at[n], device_id={'ep': partner}, device_id_type=MESH)

    def out_step(n, carry):
        wait_all(out_copies(n))
        mixed = jnp.concatenate([mix_v[i].reshape(2 * tokens, COLS) for i in range(depth)], axis=1)
        weight = pool[n, 0:depth].reshape(width, COLS)
        product = jnp.dot(mixed, weight, preferred_element_type=jnp.float32).astype(jnp.bfloat16)

        @pl.when(n >= 2)
        def _():
            store_z(n - 2).wait()
            send_z(n - 2).wait_send()

        for seq in range(2):
            resid = y_v[seq, core * blocks + n].astype(jnp.float32)
            z_v[n % 2, seq] = (resid + product[seq * tokens:(seq + 1) * tokens].astype(jnp.float32)).astype(jnp.bfloat16)
        send_z(n).start()
        store_z(n).start()
        return carry

    lax.fori_loop(0, blocks, out_step, 0)
    for n in range(blocks - 2, blocks):
        store_z(n).wait()
        send_z(n).wait_send()
    for n in range(blocks):
        send_z(n).wait_recv()
    for step in range(1, ep):
        meta_copy(step).wait_send()
    for j in range(blocks):
        swap_rows(j).wait_send()
    swap_resid.wait_send()
    for t in range(chunks):
        for pair in range(pairs):
            mix_copy(pair, t).wait_send()
    for s in range(steps):
        for part in range(2):
            y_relay(part, s).wait_send()
    for s in range(steps - 2, steps):
        for kind in range(6):
            ring_copy(kind, s).wait_send()
        for side in range(2):
            y_copy(side, s).wait_send()


def combine_and_attend(ep, pp, expert_out, expert_ids, slot_ids, gate_vals, residual, norm_scale, w_query, w_key, w_value, w_out):
    experts, cap, width = expert_out.shape
    tokens, top = expert_ids.shape
    heads, head_dim = w_query.shape[1:]
    sizes = (ep, pp, experts, cap, width, tokens, top, heads, head_dim)
    half = width // 2
    blocks = half // COLS
    chunks = tokens // CHUNK
    steps = chunks * blocks
    depth = width // COLS
    pairs = heads // 4
    chip_rows = 2 * experts * cap // ep
    any_spec = pl.BlockSpec(memory_space=pl.ANY)
    vmem_spec = pl.BlockSpec(memory_space=pltpu.VMEM)
    dma = pltpu.SemaphoreType.DMA

    def by_head(weights):
        return jnp.swapaxes(weights, 0, 1).reshape(heads, depth, COLS, head_dim)

    return pl.pallas_call(
        functools.partial(layer_kernel, sizes),
        out_shape=jax.ShapeDtypeStruct((tokens, width), jnp.bfloat16),
        in_specs=[any_spec, vmem_spec, vmem_spec, vmem_spec, any_spec, vmem_spec] + [any_spec] * 4,
        out_specs=any_spec,
        scratch_shapes=[
            pltpu.VMEM((blocks + 3 * RING_PAIRS, 2 * experts, cap, COLS), jnp.bfloat16),
            pltpu.VMEM((2, tokens, half), jnp.bfloat16),
            pltpu.VMEM((ep, 2 * top, tokens), jnp.float32),
            pltpu.VMEM((8, chunks, 3 * CHUNK, chip_rows), jnp.bfloat16),
            pltpu.VMEM((6, 2, CHUNK, COLS), jnp.float32),
            pltpu.VMEM((6, steps, CHUNK, COLS), jnp.float32),
            pltpu.VMEM((2, 2, CHUNK, COLS), jnp.bfloat16),
            pltpu.VMEM((2, depth, tokens, COLS), jnp.bfloat16),
            pltpu.VMEM((2, CHUNK, COLS), jnp.float32),
            pltpu.VMEM((2 * CHUNK, width), jnp.bfloat16),
            pltpu.VMEM((2, 2 * CHUNK, COLS), jnp.bfloat16),
            pltpu.VMEM((2, pairs, 2, tokens, COLS), jnp.bfloat16),
            pltpu.VMEM((2 * pairs, 2, tokens, COLS), jnp.bfloat16),
            pltpu.VMEM((2, 2, tokens, COLS), jnp.bfloat16),
            dma((blocks,)), dma((blocks,)), dma((blocks,)), dma, dma, dma, dma((ep - 1,)), dma((ep - 1,)),
            dma((6, steps)), dma((6, steps)), dma((2, steps)), dma((2, steps)), dma((2, steps)), dma((2, steps)),
            dma((chunks, pairs)), dma((chunks, pairs)), dma((blocks + 3 * RING_PAIRS, 2)), dma((blocks,)), dma((blocks,)), dma((blocks,)),
        ],
        compiler_params=pltpu.CompilerParams(collective_id=0, has_side_effects=True, vmem_limit_bytes=67043328),
    )(expert_out, expert_ids.T, slot_ids.T, gate_vals.T, residual, norm_scale[None],
      by_head(w_query), by_head(w_key), by_head(w_value), w_out.reshape(depth, COLS, width))


def solution(mesh):
    ep_size = mesh.shape['ep']
    pp_size = mesh.shape['pp']
    token_spec = P(('data', 'pp'), 'ep', None, None)
    weight_spec = P('pp', None, None, None)

    def body(expert_out, expert_ids, slot_ids, gate_vals, residual, norm_scale, w_query, w_key, w_value, w_out):
        result = combine_and_attend(
            ep_size, pp_size, expert_out[0], expert_ids[0, 0], slot_ids[0, 0], gate_vals[0, 0], residual[0, 0],
            norm_scale[0], w_query[0], w_key[0], w_value[0], w_out[0])
        return result[None, None]

    return jax.shard_map(body, mesh=mesh, in_specs=(token_spec, token_spec, token_spec, token_spec, token_spec, P('pp', None), weight_spec, weight_spec, weight_spec, weight_spec), out_specs=token_spec, check_vma=False)
```

```python
import functools

import jax
import jax.numpy as jnp
from jax import lax
from jax.experimental import pallas as pl
from jax.experimental.pallas import tpu as pltpu
from jax.sharding import PartitionSpec as P

NORM_EPS = 1e-6
COLS = 256
CHUNK = 192
RING_PAIRS = 3
MESH = pl.DeviceIdType.MESH


def layer_kernel(sizes, o_hbm, ids, slots, gates, h_hbm, scale_ref, wq_hbm, wk_hbm, wv_hbm, wo_hbm, z_out,
                 pool, resid_v, meta, gate_mats, send_v, recv_v, ysend_v, y_v, square_v, x_v, q_v, kv_v, mix_v, z_v,
                 rows_loc, rows_ss, rows_rs, res_loc, res_ss, res_rs, meta_ss, meta_rs,
                 ring_ss, ring_rs, y_ss, y_rs, relay_ss, relay_rs, mix_ss, mix_rs, w_sem, z_sem, zr_ss, zr_rs):
    ep, pp, experts, cap, width, tokens, top, heads, head_dim = sizes
    chips = ep // 2
    half = width // 2
    blocks = half // COLS
    chunks = tokens // CHUNK
    steps = chunks * blocks
    depth = width // COLS
    pairs = heads // 4
    cap_dev = cap // ep
    chip_rows = 2 * experts * cap_dev
    me = lax.axis_index('ep')
    stage = lax.axis_index('pp')
    chip, core = me // 2, me % 2
    partner = chip * 2 + (1 - core)
    ahead, behind, across = (chip + 1) % chips, (chip + chips - 1) % chips, (chip + 2) % chips
    next_stage, prev_stage = (stage + 1) % pp, (stage + pp - 1) % pp
    right, left = 2 * ahead + core, 2 * behind + core
    owners = (2 * across, 2 * across + 1, 2 * ahead + 1, 2 * behind, 2 * ahead, 2 * behind + 1, 2 * chip, 2 * chip + 1)

    def span(t):
        return pl.ds(pl.multiple_of(t * CHUNK, CHUNK), CHUNK)

    def lanes_at(start, size=COLS):
        return pl.ds(pl.multiple_of(start, 128), size)

    def local_rows(j):
        return pltpu.make_async_copy(o_hbm.at[:, :, lanes_at(core * half + j * COLS)],
                                     pool.at[j, pl.ds(core * experts, experts)], rows_loc.at[j])

    def swap_rows(j):
        return pltpu.make_async_remote_copy(
            src_ref=o_hbm.at[:, :, lanes_at((1 - core) * half + j * COLS)], dst_ref=pool.at[j, pl.ds(core * experts, experts)],
            send_sem=rows_ss.at[j], recv_sem=rows_rs.at[j], device_id={'ep': partner}, device_id_type=MESH)

    local_resid = pltpu.make_async_copy(h_hbm.at[:, lanes_at(core * half, half)], resid_v.at[core], res_loc)
    swap_resid = pltpu.make_async_remote_copy(
        src_ref=h_hbm.at[:, lanes_at((1 - core) * half, half)], dst_ref=resid_v.at[core],
        send_sem=res_ss, recv_sem=res_rs, device_id={'ep': partner}, device_id_type=MESH)

    def meta_copy(step):
        return pltpu.make_async_remote_copy(
            src_ref=meta.at[me], dst_ref=meta.at[me], send_sem=meta_ss.at[step - 1], recv_sem=meta_rs.at[step - 1],
            device_id={'ep': (me + step) % ep}, device_id_type=MESH)

    def ring_copy(kind, s):
        target = right if kind % 2 == 0 else left
        return pltpu.make_async_remote_copy(
            src_ref=send_v.at[kind, s % 2], dst_ref=recv_v.at[kind, s], send_sem=ring_ss.at[kind, s],
            recv_sem=ring_rs.at[kind, s], device_id={'ep': target}, device_id_type=MESH)

    def y_copy(side, s):
        return pltpu.make_async_remote_copy(
            src_ref=ysend_v.at[side, s % 2], dst_ref=y_v.at[side, core * blocks + s % blocks, span(s // blocks)],
            send_sem=y_ss.at[side, s], recv_sem=y_rs.at[core, s],
            device_id={'pp': next_stage, 'ep': 2 * chip + side}, device_id_type=MESH)

    def y_relay(part, s):
        piece = y_v.at[core, part * blocks + s % blocks, span(s // blocks)]
        return pltpu.make_async_remote_copy(
            src_ref=piece, dst_ref=piece, send_sem=relay_ss.at[part, s], recv_sem=relay_rs.at[part, s],
            device_id={'ep': partner}, device_id_type=MESH)

    def mix_copy(pair, t):
        block = mix_v.at[core * pairs + pair, :, span(t)]
        return pltpu.make_async_remote_copy(
            src_ref=block, dst_ref=block, send_sem=mix_ss.at[t, pair], recv_sem=mix_rs.at[t, pair],
            device_id={'ep': partner}, device_id_type=MESH)

    def qkv_copies(which, pair, slot):
        w_hbm = (wq_hbm, wk_hbm, wv_hbm)[which]
        return [pltpu.make_async_copy(w_hbm.at[2 * (core * pairs + pair) + i],
                                      pool.at[slot, 0:depth, :, i * head_dim:(i + 1) * head_dim], w_sem.at[slot, i]) for i in range(2)]

    def out_copies(n):
        mid = depth // 2
        return [pltpu.make_async_copy(wo_hbm.at[i * mid:(i + 1) * mid, :, lanes_at(core * half + n * COLS)],
                                      pool.at[n, i * mid:(i + 1) * mid], w_sem.at[n, i]) for i in range(2)]

    def slot_of(which, pair):
        return blocks + pair % RING_PAIRS * 3 + which

    def start_all(copies):
        for copy in copies:
            copy.start()

    def wait_all(copies):
        for copy in copies:
            copy.wait()

    for j in range(blocks):
        local_rows(j).start()
    local_resid.start()
    row_ids = jnp.where(slots[...] >= 0, ids[...] * cap_dev + slots[...] - me * cap_dev, -1)
    meta[me, 0:top, :] = row_ids.astype(jnp.float32)
    meta[me, top:2 * top, :] = gates[...]

    barrier = pltpu.get_barrier_semaphore()
    for step in range(1, ep):
        pl.semaphore_signal(barrier, inc=1, device_id={'ep': (me + step) % ep}, device_id_type=MESH)
    for side in range(2):
        pl.semaphore_signal(barrier, inc=1, device_id={'pp': next_stage, 'ep': 2 * chip + side}, device_id_type=MESH)
        pl.semaphore_signal(barrier, inc=1, device_id={'pp': prev_stage, 'ep': 2 * chip + side}, device_id_type=MESH)
    pl.semaphore_wait(barrier, ep - 1 + 4)

    for step in range(1, ep):
        meta_copy(step).start()
    for j in range(blocks):
        swap_rows(j).start()
    swap_resid.start()

    def build_gates(role):
        table = jnp.transpose(meta[owners[role]])
        wanted = (lax.broadcasted_iota(jnp.int32, (tokens, chip_rows), 1) + chip * chip_rows).astype(jnp.float32)
        total = jnp.zeros((tokens, chip_rows), jnp.float32)
        for t in range(top):
            total = total + jnp.where(table[:, t:t + 1] == wanted, table[:, top + t:top + t + 1], 0.0)
        high = total.astype(jnp.bfloat16)
        rest = total - high.astype(jnp.float32)
        mid = rest.astype(jnp.bfloat16)
        low = (rest - mid.astype(jnp.float32)).astype(jnp.bfloat16)
        for t in range(chunks):
            for i, term in enumerate((high, mid, low)):
                gate_mats[role, t, i * CHUNK:(i + 1) * CHUNK] = term[t * CHUNK:(t + 1) * CHUNK]

    def contribution(role, s):
        slot0 = pl.multiple_of(owners[role] * cap_dev, cap_dev)
        rows = pool[s % blocks, :, pl.ds(slot0, cap_dev), :].reshape(chip_rows, COLS)
        parts = jnp.dot(gate_mats[role, s // blocks], rows, preferred_element_type=jnp.float32)
        return parts[2 * CHUNK:] + parts[CHUNK:2 * CHUNK] + parts[:CHUNK]

    def leaf(kind, s):
        @pl.when(s >= 2)
        def _():
            ring_copy(kind, s - 2).wait_send()

        send_v[kind, s % 2] = contribution(kind, s)
        ring_copy(kind, s).start()

    def forward(kind, s):
        own = contribution(kind, s)

        @pl.when(s >= 2)
        def _():
            ring_copy(kind, s - 2).wait_send()

        ring_copy(kind - 4, s).wait_recv()
        send_v[kind, s % 2] = own + recv_v[kind - 4, s]
        ring_copy(kind, s).start()

    def finish(side, s):
        near, far = ((3, 4), (2, 5))[side]
        own = contribution(6 + side, s)

        @pl.when(s >= 2)
        def _():
            y_copy(side, s - 2).wait_send()

        ring_copy(near, s).wait_recv()
        ring_copy(far, s).wait_recv()
        resid = resid_v[side, span(s // blocks), lanes_at(s % blocks * COLS)].astype(jnp.float32)
        ysend_v[side, s % 2] = (resid + (own + recv_v[near, s] + recv_v[far, s])).astype(jnp.bfloat16)
        y_copy(side, s).start()

    def pass_on(s):
        for part in range(2):
            pltpu.make_async_copy(ysend_v.at[0, 0], ysend_v.at[0, 0], y_rs.at[part, s]).wait()
            y_relay(part, s).start()

    def take(s):
        @pl.when(s % blocks == 0)
        def _():
            square_v[...] = jnp.zeros_like(square_v)

        for part in range(2):
            y_relay(part, s).wait_recv()
            for seq in range(2):
                piece = y_v[seq, part * blocks + s % blocks, span(s // blocks)].astype(jnp.float32)
                square_v[seq] += piece * piece

    def normalize(t):
        for seq in range(2):
            mean = jnp.sum(square_v[seq], axis=-1, keepdims=True) / width
            inv_rms = lax.rsqrt(mean + NORM_EPS)
            for i in range(depth):
                cols = slice(i * COLS, (i + 1) * COLS)
                x_v[seq * CHUNK:(seq + 1) * CHUNK, cols] = (
                    y_v[seq, i, span(t)].astype(jnp.float32) * inv_rms * scale_ref[:, cols]).astype(jnp.bfloat16)

    def fetch(pair):
        for which in range(3):
            start_all(qkv_copies(which, pair, slot_of(which, pair)))

    def wait_pair(i, pair, t):
        @pl.when(jnp.logical_or(t == 0, i >= RING_PAIRS))
        def _():
            for which in range(3):
                wait_all(qkv_copies(which, 0, slot_of(which, pair)))

    def refill(pair, t):
        odd = t % 2
        later = pair + (1 - 2 * odd) * RING_PAIRS

        @pl.when(jnp.logical_and(later >= 0, later < pairs))
        def _():
            fetch(later)

    def project(pair, t):
        for which in range(3):
            weight = pool[slot_of(which, pair), 0:depth].reshape(width, COLS)
            product = jnp.dot(x_v[...], weight, preferred_element_type=jnp.float32).astype(jnp.bfloat16)
            if which == 0:
                q_v[pair % 2] = product
            else:
                for seq in range(2):
                    kv_v[which - 1, pair, seq, span(t)] = product[seq * CHUNK:(seq + 1) * CHUNK]

    def attend(pair, t):
        causal = (lax.broadcasted_iota(jnp.int32, (CHUNK, tokens), 0) + t * CHUNK
                  >= lax.broadcasted_iota(jnp.int32, (CHUNK, tokens), 1))
        mixed = []
        for seq in range(2):
            for i in range(2):
                lanes = slice(i * head_dim, (i + 1) * head_dim)
                q = q_v[pair % 2, seq * CHUNK:(seq + 1) * CHUNK, lanes]
                k, v = kv_v[0, pair, seq, :, lanes], kv_v[1, pair, seq, :, lanes]
                scores = lax.dot_general(q, k, (((1,), (1,)), ((), ())), preferred_element_type=jnp.float32) * head_dim ** -0.5
                scores = jnp.where(causal, scores, -1e30)
                exps = jnp.exp(scores - jnp.max(scores, axis=-1, keepdims=True))
                sums = jnp.sum(exps, axis=-1, keepdims=True)
                mixed.append((jnp.dot(exps.astype(jnp.bfloat16), v, preferred_element_type=jnp.float32) / sums).astype(jnp.bfloat16))
        return mixed

    def store_mixed(pair, t, mixed):
        for seq in range(2):
            for i in range(2):
                mix_v[core * pairs + pair, seq, span(t), i * head_dim:(i + 1) * head_dim] = mixed[2 * seq + i]
        mix_copy(pair, t).start()

    for step in range(1, ep):
        meta_copy(step).wait_recv()

    def ring_step(s, carry):
        @pl.when(s < steps)
        def _():
            @pl.when(s < blocks)
            def _():
                local_rows(s).wait()
                swap_rows(s).wait_recv()

            for kind in range(4):
                @pl.when(s == 0)
                def _():
                    build_gates(kind)

                leaf(kind, s)

        @pl.when(s == 0)
        def _():
            for role in range(4, 8):
                build_gates(role)
            local_resid.wait()
            swap_resid.wait_recv()
            kv_v[...] = jnp.zeros_like(kv_v)

        for which in range(3):
            @pl.when(jnp.logical_and(s % 3 == which, s < 3 * RING_PAIRS))
            def _():
                start_all(qkv_copies(which, s // 3, slot_of(which, s // 3)))

        @pl.when(jnp.logical_and(s >= 1, s < steps + 1))
        def _():
            forward(4, s - 1)
            forward(5, s - 1)

        lag = s % blocks - 4

        @pl.when(jnp.logical_and(jnp.logical_and(s >= blocks, s < steps), lag >= 0))
        def _():
            def one_pair(i, carry):
                t = s // blocks - 1
                odd = t % 2
                pair = odd * (pairs - 1) + (1 - 2 * odd) * i
                wait_pair(i, pair, t)
                project(pair, t)
                refill(pair, t)
                store_mixed(pair, t, attend(pair, t))
                return carry

            lax.fori_loop(3 * lag, jnp.minimum(3 * lag + 3, pairs), one_pair, 0)

        @pl.when(jnp.logical_and(s >= 2, s < steps + 2))
        def _():
            finish(0, s - 2)
            finish(1, s - 2)

            @pl.when(s - 2 >= steps - blocks)
            def _():
                start_all(out_copies(s - 2 - (steps - blocks)))

        @pl.when(jnp.logical_and(s >= 3, s < steps + 3))
        def _():
            pass_on(s - 3)

        @pl.when(s >= 4)
        def _():
            take(s - 4)

        @pl.when(jnp.logical_and(s >= blocks, s % blocks == 3))
        def _():
            normalize(s // blocks - 1)

        return carry

    lax.fori_loop(0, steps + 4, ring_step, 0)

    last = chunks - 1
    flip = last % 2

    def nth(i):
        return pairs - 1 - i if flip else i

    wait_pair(0, nth(0), last)
    project(nth(0), last)
    refill(nth(0), last)

    def pair_step(i, carry):
        wait_pair(i, nth(i), last)
        mixed = attend(nth(i - 1), last)
        project(nth(i), last)
        store_mixed(nth(i - 1), last, mixed)
        refill(nth(i), last)
        return carry

    lax.fori_loop(1, pairs, pair_step, 0)
    store_mixed(nth(pairs - 1), last, attend(nth(pairs - 1), last))

    for t in range(chunks):
        for pair in range(pairs):
            mix_copy(pair, t).wait_recv()

    def store_z(n):
        return pltpu.make_async_copy(z_v.at[n % 2, core], z_out.at[:, lanes_at(core * half + n * COLS)], z_sem.at[n])

    def send_z(n):
        return pltpu.make_async_remote_copy(
            src_ref=z_v.at[n % 2, 1 - core], dst_ref=z_out.at[:, lanes_at(core * half + n * COLS)],
            send_sem=zr_ss.at[n], recv_sem=zr_rs.at[n], device_id={'ep': partner}, device_id_type=MESH)

    def out_step(n, carry):
        wait_all(out_copies(n))
        mixed = jnp.concatenate([mix_v[i].reshape(2 * tokens, COLS) for i in range(depth)], axis=1)
        weight = pool[n, 0:depth].reshape(width, COLS)
        product = jnp.dot(mixed, weight, preferred_element_type=jnp.float32).astype(jnp.bfloat16)

        @pl.when(n >= 2)
        def _():
            store_z(n - 2).wait()
            send_z(n - 2).wait_send()

        for seq in range(2):
            resid = y_v[seq, core * blocks + n].astype(jnp.float32)
            z_v[n % 2, seq] = (resid + product[seq * tokens:(seq + 1) * tokens].astype(jnp.float32)).astype(jnp.bfloat16)
        send_z(n).start()
        store_z(n).start()
        return carry

    lax.fori_loop(0, blocks, out_step, 0)
    for n in range(blocks - 2, blocks):
        store_z(n).wait()
        send_z(n).wait_send()
    for n in range(blocks):
        send_z(n).wait_recv()
    for step in range(1, ep):
        meta_copy(step).wait_send()
    for j in range(blocks):
        swap_rows(j).wait_send()
    swap_resid.wait_send()
    for t in range(chunks):
        for pair in range(pairs):
            mix_copy(pair, t).wait_send()
    for s in range(steps):
        for part in range(2):
            y_relay(part, s).wait_send()
    for s in range(steps - 2, steps):
        for kind in range(6):
            ring_copy(kind, s).wait_send()
        for side in range(2):
            y_copy(side, s).wait_send()


def combine_and_attend(ep, pp, expert_out, expert_ids, slot_ids, gate_vals, residual, norm_scale, w_query, w_key, w_value, w_out):
    experts, cap, width = expert_out.shape
    tokens, top = expert_ids.shape
    heads, head_dim = w_query.shape[1:]
    sizes = (ep, pp, experts, cap, width, tokens, top, heads, head_dim)
    half = width // 2
    blocks = half // COLS
    chunks = tokens // CHUNK
    steps = chunks * blocks
    depth = width // COLS
    pairs = heads // 4
    chip_rows = 2 * experts * cap // ep
    any_spec = pl.BlockSpec(memory_space=pl.ANY)
    vmem_spec = pl.BlockSpec(memory_space=pltpu.VMEM)
    dma = pltpu.SemaphoreType.DMA

    def by_head(weights):
        return jnp.swapaxes(weights, 0, 1).reshape(heads, depth, COLS, head_dim)

    return pl.pallas_call(
        functools.partial(layer_kernel, sizes),
        out_shape=jax.ShapeDtypeStruct((tokens, width), jnp.bfloat16),
        in_specs=[any_spec, vmem_spec, vmem_spec, vmem_spec, any_spec, vmem_spec] + [any_spec] * 4,
        out_specs=any_spec,
        scratch_shapes=[
            pltpu.VMEM((blocks + 3 * RING_PAIRS, 2 * experts, cap, COLS), jnp.bfloat16),
            pltpu.VMEM((2, tokens, half), jnp.bfloat16),
            pltpu.VMEM((ep, 2 * top, tokens), jnp.float32),
            pltpu.VMEM((8, chunks, 3 * CHUNK, chip_rows), jnp.bfloat16),
            pltpu.VMEM((6, 2, CHUNK, COLS), jnp.float32),
            pltpu.VMEM((6, steps, CHUNK, COLS), jnp.float32),
            pltpu.VMEM((2, 2, CHUNK, COLS), jnp.bfloat16),
            pltpu.VMEM((2, depth, tokens, COLS), jnp.bfloat16),
            pltpu.VMEM((2, CHUNK, COLS), jnp.float32),
            pltpu.VMEM((2 * CHUNK, width), jnp.bfloat16),
            pltpu.VMEM((2, 2 * CHUNK, COLS), jnp.bfloat16),
            pltpu.VMEM((2, pairs, 2, tokens, COLS), jnp.bfloat16),
            pltpu.VMEM((2 * pairs, 2, tokens, COLS), jnp.bfloat16),
            pltpu.VMEM((2, 2, tokens, COLS), jnp.bfloat16),
            dma((blocks,)), dma((blocks,)), dma((blocks,)), dma, dma, dma, dma((ep - 1,)), dma((ep - 1,)),
            dma((6, steps)), dma((6, steps)), dma((2, steps)), dma((2, steps)), dma((2, steps)), dma((2, steps)),
            dma((chunks, pairs)), dma((chunks, pairs)), dma((blocks + 3 * RING_PAIRS, 2)), dma((blocks,)), dma((blocks,)), dma((blocks,)),
        ],
        compiler_params=pltpu.CompilerParams(collective_id=0, has_side_effects=True, vmem_limit_bytes=67043328),
    )(expert_out, expert_ids.T, slot_ids.T, gate_vals.T, residual, norm_scale[None],
      by_head(w_query), by_head(w_key), by_head(w_value), w_out.reshape(depth, COLS, width))


def solution(mesh):
    ep_size = mesh.shape['ep']
    pp_size = mesh.shape['pp']
    token_spec = P(('data', 'pp'), 'ep', None, None)
    weight_spec = P('pp', None, None, None)

    def body(expert_out, expert_ids, slot_ids, gate_vals, residual, norm_scale, w_query, w_key, w_value, w_out):
        result = combine_and_attend(
            ep_size, pp_size, expert_out[0], expert_ids[0, 0], slot_ids[0, 0], gate_vals[0, 0], residual[0, 0],
            norm_scale[0], w_query[0], w_key[0], w_value[0], w_out[0])
        return result[None, None]

    return jax.shard_map(body, mesh=mesh, in_specs=(token_spec, token_spec, token_spec, token_spec, token_spec, P('pp', None), weight_spec, weight_spec, weight_spec, weight_spec), out_specs=token_spec, check_vma=False)
```

```python
import functools

import jax
import jax.numpy as jnp
from jax import lax
from jax.experimental import pallas as pl
from jax.experimental.pallas import tpu as pltpu
from jax.sharding import PartitionSpec as P

NORM_EPS = 1e-6
COLS = 256
CHUNK = 192
RING_PAIRS = 3
MESH = pl.DeviceIdType.MESH


def layer_kernel(sizes, o_hbm, ids, slots, gates, h_hbm, scale_ref, wq_hbm, wk_hbm, wv_hbm, wo_hbm, z_out,
                 pool, resid_v, meta, gate_mats, send_v, recv_v, ysend_v, y_v, square_v, x_v, q_v, kv_v, mix_v, z_v,
                 rows_loc, rows_ss, rows_rs, res_loc, res_ss, res_rs, meta_ss, meta_rs,
                 ring_ss, ring_rs, y_ss, y_rs, relay_ss, relay_rs, mix_ss, mix_rs, w_sem, z_sem, zr_ss, zr_rs):
    ep, pp, experts, cap, width, tokens, top, heads, head_dim = sizes
    chips = ep // 2
    half = width // 2
    blocks = half // COLS
    chunks = tokens // CHUNK
    steps = chunks * blocks
    depth = width // COLS
    pairs = heads // 4
    cap_dev = cap // ep
    chip_rows = 2 * experts * cap_dev
    me = lax.axis_index('ep')
    stage = lax.axis_index('pp')
    chip, core = me // 2, me % 2
    partner = chip * 2 + (1 - core)
    ahead, behind, across = (chip + 1) % chips, (chip + chips - 1) % chips, (chip + 2) % chips
    next_stage, prev_stage = (stage + 1) % pp, (stage + pp - 1) % pp
    right, left = 2 * ahead + core, 2 * behind + core
    owners = (2 * across, 2 * across + 1, 2 * ahead + 1, 2 * behind, 2 * ahead, 2 * behind + 1, 2 * chip, 2 * chip + 1)

    def span(t):
        return pl.ds(pl.multiple_of(t * CHUNK, CHUNK), CHUNK)

    def lanes_at(start, size=COLS):
        return pl.ds(pl.multiple_of(start, 128), size)

    def local_rows(j):
        return pltpu.make_async_copy(o_hbm.at[:, :, lanes_at(core * half + j * COLS)],
                                     pool.at[j, pl.ds(core * experts, experts)], rows_loc.at[j])

    def swap_rows(j):
        return pltpu.make_async_remote_copy(
            src_ref=o_hbm.at[:, :, lanes_at((1 - core) * half + j * COLS)], dst_ref=pool.at[j, pl.ds(core * experts, experts)],
            send_sem=rows_ss.at[j], recv_sem=rows_rs.at[j], device_id={'ep': partner}, device_id_type=MESH)

    local_resid = pltpu.make_async_copy(h_hbm.at[:, lanes_at(core * half, half)], resid_v.at[core], res_loc)
    swap_resid = pltpu.make_async_remote_copy(
        src_ref=h_hbm.at[:, lanes_at((1 - core) * half, half)], dst_ref=resid_v.at[core],
        send_sem=res_ss, recv_sem=res_rs, device_id={'ep': partner}, device_id_type=MESH)

    def meta_copy(step):
        return pltpu.make_async_remote_copy(
            src_ref=meta.at[me], dst_ref=meta.at[me], send_sem=meta_ss.at[step - 1], recv_sem=meta_rs.at[step - 1],
            device_id={'ep': (me + step) % ep}, device_id_type=MESH)

    def ring_copy(kind, s):
        target = right if kind % 2 == 0 else left
        return pltpu.make_async_remote_copy(
            src_ref=send_v.at[kind, s % 2], dst_ref=recv_v.at[kind, s], send_sem=ring_ss.at[kind, s],
            recv_sem=ring_rs.at[kind, s], device_id={'ep': target}, device_id_type=MESH)

    def y_copy(side, s):
        return pltpu.make_async_remote_copy(
            src_ref=ysend_v.at[side, s % 2], dst_ref=y_v.at[side, core * blocks + s % blocks, span(s // blocks)],
            send_sem=y_ss.at[side, s], recv_sem=y_rs.at[core, s],
            device_id={'pp': next_stage, 'ep': 2 * chip + side}, device_id_type=MESH)

    def y_relay(part, s):
        piece = y_v.at[core, part * blocks + s % blocks, span(s // blocks)]
        return pltpu.make_async_remote_copy(
            src_ref=piece, dst_ref=piece, send_sem=relay_ss.at[part, s], recv_sem=relay_rs.at[part, s],
            device_id={'ep': partner}, device_id_type=MESH)

    def mix_copy(pair, t):
        block = mix_v.at[core * pairs + pair, :, span(t)]
        return pltpu.make_async_remote_copy(
            src_ref=block, dst_ref=block, send_sem=mix_ss.at[t, pair], recv_sem=mix_rs.at[t, pair],
            device_id={'ep': partner}, device_id_type=MESH)

    def qkv_copies(which, pair, slot):
        w_hbm = (wq_hbm, wk_hbm, wv_hbm)[which]
        return [pltpu.make_async_copy(w_hbm.at[2 * (core * pairs + pair) + i],
                                      pool.at[slot, 0:depth, :, i * head_dim:(i + 1) * head_dim], w_sem.at[slot, i]) for i in range(2)]

    def out_copies(n):
        mid = depth // 2
        return [pltpu.make_async_copy(wo_hbm.at[i * mid:(i + 1) * mid, :, lanes_at(core * half + n * COLS)],
                                      pool.at[n, i * mid:(i + 1) * mid], w_sem.at[n, i]) for i in range(2)]

    def slot_of(which, pair):
        return blocks + pair % RING_PAIRS * 3 + which

    def start_all(copies):
        for copy in copies:
            copy.start()

    def wait_all(copies):
        for copy in copies:
            copy.wait()

    local_rows(0).start()
    row_ids = jnp.where(slots[...] >= 0, ids[...] * cap_dev + slots[...] - me * cap_dev, -1)
    meta[me, 0:top, :] = row_ids.astype(jnp.float32)
    meta[me, top:2 * top, :] = gates[...]

    barrier = pltpu.get_barrier_semaphore()
    for step in range(1, ep):
        pl.semaphore_signal(barrier, inc=1, device_id={'ep': (me + step) % ep}, device_id_type=MESH)
    for side in range(2):
        pl.semaphore_signal(barrier, inc=1, device_id={'pp': next_stage, 'ep': 2 * chip + side}, device_id_type=MESH)
        pl.semaphore_signal(barrier, inc=1, device_id={'pp': prev_stage, 'ep': 2 * chip + side}, device_id_type=MESH)
    pl.semaphore_wait(barrier, ep - 1 + 4)

    for step in range(1, ep):
        meta_copy(step).start()
    swap_rows(0).start()
    for j in range(1, blocks):
        local_rows(j).start()
        swap_rows(j).start()
    local_resid.start()
    swap_resid.start()

    def build_gates(role):
        table = jnp.transpose(meta[owners[role]])
        wanted = (lax.broadcasted_iota(jnp.int32, (tokens, chip_rows), 1) + chip * chip_rows).astype(jnp.float32)
        total = jnp.zeros((tokens, chip_rows), jnp.float32)
        for t in range(top):
            total = total + jnp.where(table[:, t:t + 1] == wanted, table[:, top + t:top + t + 1], 0.0)
        high = total.astype(jnp.bfloat16)
        rest = total - high.astype(jnp.float32)
        mid = rest.astype(jnp.bfloat16)
        low = (rest - mid.astype(jnp.float32)).astype(jnp.bfloat16)
        for t in range(chunks):
            for i, term in enumerate((high, mid, low)):
                gate_mats[role, t, i * CHUNK:(i + 1) * CHUNK] = term[t * CHUNK:(t + 1) * CHUNK]

    def contribution(role, s):
        slot0 = pl.multiple_of(owners[role] * cap_dev, cap_dev)
        rows = pool[s % blocks, :, pl.ds(slot0, cap_dev), :].reshape(chip_rows, COLS)
        parts = jnp.dot(gate_mats[role, s // blocks], rows, preferred_element_type=jnp.float32)
        return parts[2 * CHUNK:] + parts[CHUNK:2 * CHUNK] + parts[:CHUNK]

    def leaf(kind, s):
        @pl.when(s >= 2)
        def _():
            ring_copy(kind, s - 2).wait_send()

        send_v[kind, s % 2] = contribution(kind, s)
        ring_copy(kind, s).start()

    def forward(kind, s):
        own = contribution(kind, s)

        @pl.when(s >= 2)
        def _():
            ring_copy(kind, s - 2).wait_send()

        ring_copy(kind - 4, s).wait_recv()
        send_v[kind, s % 2] = own + recv_v[kind - 4, s]
        ring_copy(kind, s).start()

    def finish(side, s):
        near, far = ((3, 4), (2, 5))[side]
        own = contribution(6 + side, s)

        @pl.when(s >= 2)
        def _():
            y_copy(side, s - 2).wait_send()

        ring_copy(near, s).wait_recv()
        ring_copy(far, s).wait_recv()
        resid = resid_v[side, span(s // blocks), lanes_at(s % blocks * COLS)].astype(jnp.float32)
        ysend_v[side, s % 2] = (resid + (own + recv_v[near, s] + recv_v[far, s])).astype(jnp.bfloat16)
        y_copy(side, s).start()

    def pass_on(s):
        for part in range(2):
            pltpu.make_async_copy(ysend_v.at[0, 0], ysend_v.at[0, 0], y_rs.at[part, s]).wait()
            y_relay(part, s).start()

    def take(s):
        @pl.when(s % blocks == 0)
        def _():
            square_v[...] = jnp.zeros_like(square_v)

        for part in range(2):
            y_relay(part, s).wait_recv()
            for seq in range(2):
                piece = y_v[seq, part * blocks + s % blocks, span(s // blocks)].astype(jnp.float32)
                square_v[seq] += piece * piece

    def normalize(t):
        for seq in range(2):
            mean = jnp.sum(square_v[seq], axis=-1, keepdims=True) / width
            inv_rms = lax.rsqrt(mean + NORM_EPS)
            for i in range(depth):
                cols = slice(i * COLS, (i + 1) * COLS)
                x_v[seq * CHUNK:(seq + 1) * CHUNK, cols] = (
                    y_v[seq, i, span(t)].astype(jnp.float32) * inv_rms * scale_ref[:, cols]).astype(jnp.bfloat16)

    def fetch(pair):
        for which in range(3):
            start_all(qkv_copies(which, pair, slot_of(which, pair)))

    def wait_pair(i, pair, t):
        @pl.when(jnp.logical_or(t == 0, i >= RING_PAIRS))
        def _():
            for which in range(3):
                wait_all(qkv_copies(which, 0, slot_of(which, pair)))

    def refill(pair, t):
        odd = t % 2
        later = pair + (1 - 2 * odd) * RING_PAIRS

        @pl.when(jnp.logical_and(later >= 0, later < pairs))
        def _():
            fetch(later)

    def project(pair, t):
        for which in range(3):
            weight = pool[slot_of(which, pair), 0:depth].reshape(width, COLS)
            product = jnp.dot(x_v[...], weight, preferred_element_type=jnp.float32).astype(jnp.bfloat16)
            if which == 0:
                q_v[pair % 2] = product
            else:
                for seq in range(2):
                    kv_v[which - 1, pair, seq, span(t)] = product[seq * CHUNK:(seq + 1) * CHUNK]

    def attend(pair, t):
        causal = (lax.broadcasted_iota(jnp.int32, (CHUNK, tokens), 0) + t * CHUNK
                  >= lax.broadcasted_iota(jnp.int32, (CHUNK, tokens), 1))
        mixed = []
        for seq in range(2):
            for i in range(2):
                lanes = slice(i * head_dim, (i + 1) * head_dim)
                q = q_v[pair % 2, seq * CHUNK:(seq + 1) * CHUNK, lanes]
                k, v = kv_v[0, pair, seq, :, lanes], kv_v[1, pair, seq, :, lanes]
                scores = lax.dot_general(q, k, (((1,), (1,)), ((), ())), preferred_element_type=jnp.float32) * head_dim ** -0.5
                scores = jnp.where(causal, scores, -1e30)
                exps = jnp.exp(scores - jnp.max(scores, axis=-1, keepdims=True))
                sums = jnp.sum(exps, axis=-1, keepdims=True)
                mixed.append((jnp.dot(exps.astype(jnp.bfloat16), v, preferred_element_type=jnp.float32) / sums).astype(jnp.bfloat16))
        return mixed

    def store_mixed(pair, t, mixed):
        for seq in range(2):
            for i in range(2):
                mix_v[core * pairs + pair, seq, span(t), i * head_dim:(i + 1) * head_dim] = mixed[2 * seq + i]
        mix_copy(pair, t).start()

    for step in range(1, ep):
        meta_copy(step).wait_recv()

    def ring_step(s, carry):
        @pl.when(s < steps)
        def _():
            @pl.when(s < blocks)
            def _():
                local_rows(s).wait()
                swap_rows(s).wait_recv()

            for kind in range(4):
                @pl.when(s == 0)
                def _():
                    build_gates(kind)

                leaf(kind, s)

        @pl.when(s == 0)
        def _():
            for role in range(4, 8):
                build_gates(role)
            local_resid.wait()
            swap_resid.wait_recv()
            kv_v[...] = jnp.zeros_like(kv_v)

        @pl.when(jnp.logical_and(s >= 1, s < steps + 1))
        def _():
            forward(4, s - 1)
            forward(5, s - 1)

        @pl.when(jnp.logical_and(s >= 2, s < steps + 2))
        def _():
            finish(0, s - 2)
            finish(1, s - 2)

            @pl.when(s - 2 == steps - 1)
            def _():
                fetch(0)
                fetch(1)

        @pl.when(jnp.logical_and(s >= 3, s < steps + 3))
        def _():
            pass_on(s - 3)

        @pl.when(s >= 4)
        def _():
            take(s - 4)

        @pl.when(jnp.logical_and(s >= blocks, s % blocks == 3))
        def _():
            normalize(s // blocks - 1)

        return carry

    lax.fori_loop(0, steps + 4, ring_step, 0)

    for pair in range(2, RING_PAIRS):
        fetch(pair)
    last = chunks - 1
    flip = last % 2

    def nth(i):
        return pairs - 1 - i if flip else i

    wait_pair(0, nth(0), last)
    project(nth(0), last)
    refill(nth(0), last)
    start_all(out_copies(0))

    def pair_step(i, carry):
        wait_pair(i, nth(i), last)
        mixed = attend(nth(i - 1), last)
        project(nth(i), last)
        store_mixed(nth(i - 1), last, mixed)
        refill(nth(i), last)
        start_all(out_copies(i))
        return carry

    lax.fori_loop(1, pairs, pair_step, 0)
    store_mixed(nth(pairs - 1), last, attend(nth(pairs - 1), last))

    for t in range(chunks):
        for pair in range(pairs):
            mix_copy(pair, t).wait_recv()

    def store_z(n):
        return pltpu.make_async_copy(z_v.at[n % 2, core], z_out.at[:, lanes_at(core * half + n * COLS)], z_sem.at[n])

    def send_z(n):
        return pltpu.make_async_remote_copy(
            src_ref=z_v.at[n % 2, 1 - core], dst_ref=z_out.at[:, lanes_at(core * half + n * COLS)],
            send_sem=zr_ss.at[n], recv_sem=zr_rs.at[n], device_id={'ep': partner}, device_id_type=MESH)

    def out_step(n, carry):
        wait_all(out_copies(n))
        mixed = jnp.concatenate([mix_v[i].reshape(2 * tokens, COLS) for i in range(depth)], axis=1)
        weight = pool[n, 0:depth].reshape(width, COLS)
        product = jnp.dot(mixed, weight, preferred_element_type=jnp.float32).astype(jnp.bfloat16)

        @pl.when(n >= 2)
        def _():
            store_z(n - 2).wait()
            send_z(n - 2).wait_send()

        for seq in range(2):
            resid = y_v[seq, core * blocks + n].astype(jnp.float32)
            z_v[n % 2, seq] = (resid + product[seq * tokens:(seq + 1) * tokens].astype(jnp.float32)).astype(jnp.bfloat16)
        send_z(n).start()
        store_z(n).start()
        return carry

    lax.fori_loop(0, blocks, out_step, 0)
    for n in range(blocks - 2, blocks):
        store_z(n).wait()
        send_z(n).wait_send()
    for n in range(blocks):
        send_z(n).wait_recv()
    for step in range(1, ep):
        meta_copy(step).wait_send()
    for j in range(blocks):
        swap_rows(j).wait_send()
    swap_resid.wait_send()
    for t in range(chunks):
        for pair in range(pairs):
            mix_copy(pair, t).wait_send()
    for s in range(steps):
        for part in range(2):
            y_relay(part, s).wait_send()
    for s in range(steps - 2, steps):
        for kind in range(6):
            ring_copy(kind, s).wait_send()
        for side in range(2):
            y_copy(side, s).wait_send()


def combine_and_attend(ep, pp, expert_out, expert_ids, slot_ids, gate_vals, residual, norm_scale, w_query, w_key, w_value, w_out):
    experts, cap, width = expert_out.shape
    tokens, top = expert_ids.shape
    heads, head_dim = w_query.shape[1:]
    sizes = (ep, pp, experts, cap, width, tokens, top, heads, head_dim)
    half = width // 2
    blocks = half // COLS
    chunks = tokens // CHUNK
    steps = chunks * blocks
    depth = width // COLS
    pairs = heads // 4
    chip_rows = 2 * experts * cap // ep
    any_spec = pl.BlockSpec(memory_space=pl.ANY)
    vmem_spec = pl.BlockSpec(memory_space=pltpu.VMEM)
    dma = pltpu.SemaphoreType.DMA

    def by_head(weights):
        return jnp.swapaxes(weights, 0, 1).reshape(heads, depth, COLS, head_dim)

    return pl.pallas_call(
        functools.partial(layer_kernel, sizes),
        out_shape=jax.ShapeDtypeStruct((tokens, width), jnp.bfloat16),
        in_specs=[any_spec, vmem_spec, vmem_spec, vmem_spec, any_spec, vmem_spec] + [any_spec] * 4,
        out_specs=any_spec,
        scratch_shapes=[
            pltpu.VMEM((blocks + 3 * RING_PAIRS, 2 * experts, cap, COLS), jnp.bfloat16),
            pltpu.VMEM((2, tokens, half), jnp.bfloat16),
            pltpu.VMEM((ep, 2 * top, tokens), jnp.float32),
            pltpu.VMEM((8, chunks, 3 * CHUNK, chip_rows), jnp.bfloat16),
            pltpu.VMEM((6, 2, CHUNK, COLS), jnp.float32),
            pltpu.VMEM((6, steps, CHUNK, COLS), jnp.float32),
            pltpu.VMEM((2, 2, CHUNK, COLS), jnp.bfloat16),
            pltpu.VMEM((2, depth, tokens, COLS), jnp.bfloat16),
            pltpu.VMEM((2, CHUNK, COLS), jnp.float32),
            pltpu.VMEM((2 * CHUNK, width), jnp.bfloat16),
            pltpu.VMEM((2, 2 * CHUNK, COLS), jnp.bfloat16),
            pltpu.VMEM((2, pairs, 2, tokens, COLS), jnp.bfloat16),
            pltpu.VMEM((2 * pairs, 2, tokens, COLS), jnp.bfloat16),
            pltpu.VMEM((2, 2, tokens, COLS), jnp.bfloat16),
            dma((blocks,)), dma((blocks,)), dma((blocks,)), dma, dma, dma, dma((ep - 1,)), dma((ep - 1,)),
            dma((6, steps)), dma((6, steps)), dma((2, steps)), dma((2, steps)), dma((2, steps)), dma((2, steps)),
            dma((chunks, pairs)), dma((chunks, pairs)), dma((blocks + 3 * RING_PAIRS, 2)), dma((blocks,)), dma((blocks,)), dma((blocks,)),
        ],
        compiler_params=pltpu.CompilerParams(collective_id=0, has_side_effects=True, vmem_limit_bytes=67043328),
    )(expert_out, expert_ids.T, slot_ids.T, gate_vals.T, residual, norm_scale[None],
      by_head(w_query), by_head(w_key), by_head(w_value), w_out.reshape(depth, COLS, width))


def solution(mesh):
    ep_size = mesh.shape['ep']
    pp_size = mesh.shape['pp']
    token_spec = P(('data', 'pp'), 'ep', None, None)
    weight_spec = P('pp', None, None, None)

    def body(expert_out, expert_ids, slot_ids, gate_vals, residual, norm_scale, w_query, w_key, w_value, w_out):
        result = combine_and_attend(
            ep_size, pp_size, expert_out[0], expert_ids[0, 0], slot_ids[0, 0], gate_vals[0, 0], residual[0, 0],
            norm_scale[0], w_query[0], w_key[0], w_value[0], w_out[0])
        return result[None, None]

    return jax.shard_map(body, mesh=mesh, in_specs=(token_spec, token_spec, token_spec, token_spec, token_spec, P('pp', None), weight_spec, weight_spec, weight_spec, weight_spec), out_specs=token_spec, check_vma=False)
```

```python
import functools

import jax
import jax.numpy as jnp
from jax import lax
from jax.experimental import pallas as pl
from jax.experimental.pallas import tpu as pltpu
from jax.sharding import PartitionSpec as P

NORM_EPS = 1e-6
COLS = 256
CHUNK = 96
RING_PAIRS = 4
MESH = pl.DeviceIdType.MESH


def layer_kernel(sizes, o_hbm, ids, slots, gates, h_hbm, scale_ref, wq_hbm, wk_hbm, wv_hbm, wo_hbm, z_out,
                 pool, heads_v, resid_v, meta, gate_mats, send_v, recv_v, ysend_v, y_v, square_v, x_v, q_v, kv_v, mix_v, z_v,
                 rows_loc, rows_ss, rows_rs, res_loc, res_ss, res_rs, meta_ss, meta_rs,
                 ring_ss, ring_rs, y_ss, y_rs, relay_ss, relay_rs, mix_ss, mix_rs, qkv_sem, w_sem, z_sem, zr_ss, zr_rs):
    ep, pp, experts, cap, width, tokens, top, heads, head_dim = sizes
    chips = ep // 2
    half = width // 2
    blocks = half // COLS
    chunks = tokens // CHUNK
    steps = chunks * blocks
    depth = width // COLS
    pairs = heads // 4
    cap_dev = cap // ep
    chip_rows = 2 * experts * cap_dev
    me = lax.axis_index('ep')
    stage = lax.axis_index('pp')
    chip, core = me // 2, me % 2
    partner = chip * 2 + (1 - core)
    ahead, behind, across = (chip + 1) % chips, (chip + chips - 1) % chips, (chip + 2) % chips
    next_stage, prev_stage = (stage + 1) % pp, (stage + pp - 1) % pp
    right, left = 2 * ahead + core, 2 * behind + core
    owners = (2 * across, 2 * across + 1, 2 * ahead + 1, 2 * behind, 2 * ahead, 2 * behind + 1, 2 * chip, 2 * chip + 1)

    def span(t):
        return pl.ds(pl.multiple_of(t * CHUNK, CHUNK), CHUNK)

    def lanes_at(start, size=COLS):
        return pl.ds(pl.multiple_of(start, 128), size)

    def local_rows(j):
        return pltpu.make_async_copy(o_hbm.at[:, :, lanes_at(core * half + j * COLS)],
                                     pool.at[j, pl.ds(core * experts, experts)], rows_loc.at[j])

    def swap_rows(j):
        return pltpu.make_async_remote_copy(
            src_ref=o_hbm.at[:, :, lanes_at((1 - core) * half + j * COLS)], dst_ref=pool.at[j, pl.ds(core * experts, experts)],
            send_sem=rows_ss.at[j], recv_sem=rows_rs.at[j], device_id={'ep': partner}, device_id_type=MESH)

    local_resid = pltpu.make_async_copy(h_hbm.at[:, lanes_at(core * half, half)], resid_v.at[core], res_loc)
    swap_resid = pltpu.make_async_remote_copy(
        src_ref=h_hbm.at[:, lanes_at((1 - core) * half, half)], dst_ref=resid_v.at[core],
        send_sem=res_ss, recv_sem=res_rs, device_id={'ep': partner}, device_id_type=MESH)

    def meta_copy(step):
        return pltpu.make_async_remote_copy(
            src_ref=meta.at[me], dst_ref=meta.at[me], send_sem=meta_ss.at[step - 1], recv_sem=meta_rs.at[step - 1],
            device_id={'ep': (me + step) % ep}, device_id_type=MESH)

    def ring_copy(kind, s):
        target = right if kind % 2 == 0 else left
        return pltpu.make_async_remote_copy(
            src_ref=send_v.at[kind, s % 2], dst_ref=recv_v.at[kind, s], send_sem=ring_ss.at[kind, s],
            recv_sem=ring_rs.at[kind, s], device_id={'ep': target}, device_id_type=MESH)

    def y_copy(side, s):
        return pltpu.make_async_remote_copy(
            src_ref=ysend_v.at[side, s % 2], dst_ref=y_v.at[side, core * blocks + s % blocks, span(s // blocks)],
            send_sem=y_ss.at[side, s], recv_sem=y_rs.at[core, s],
            device_id={'pp': next_stage, 'ep': 2 * chip + side}, device_id_type=MESH)

    def y_relay(part, s):
        piece = y_v.at[core, part * blocks + s % blocks, span(s // blocks)]
        return pltpu.make_async_remote_copy(
            src_ref=piece, dst_ref=piece, send_sem=relay_ss.at[part, s], recv_sem=relay_rs.at[part, s],
            device_id={'ep': partner}, device_id_type=MESH)

    def mix_copy(pair, t):
        block = mix_v.at[core * pairs + pair, :, span(t)]
        return pltpu.make_async_remote_copy(
            src_ref=block, dst_ref=block, send_sem=mix_ss.at[t, pair], recv_sem=mix_rs.at[t, pair],
            device_id={'ep': partner}, device_id_type=MESH)

    def qkv_copies(which, pair, slot):
        w_hbm = (wq_hbm, wk_hbm, wv_hbm)[which]
        return [pltpu.make_async_copy(w_hbm.at[2 * (core * pairs + pair) + i],
                                      heads_v.at[slot, i], qkv_sem.at[slot, i]) for i in range(2)]

    def out_copies(n):
        mid = depth // 2
        return [pltpu.make_async_copy(wo_hbm.at[i * mid:(i + 1) * mid, :, lanes_at(core * half + n * COLS)],
                                      pool.at[n, i * mid:(i + 1) * mid], w_sem.at[n, i]) for i in range(2)]

    def slot_of(which, pair):
        return pair % RING_PAIRS * 3 + which

    def start_all(copies):
        for copy in copies:
            copy.start()

    def wait_all(copies):
        for copy in copies:
            copy.wait()

    for j in range(blocks):
        local_rows(j).start()
    local_resid.start()
    row_ids = jnp.where(slots[...] >= 0, ids[...] * cap_dev + slots[...] - me * cap_dev, -1)
    meta[me, 0:top, :] = row_ids.astype(jnp.float32)
    meta[me, top:2 * top, :] = gates[...]

    barrier = pltpu.get_barrier_semaphore()
    for step in range(1, ep):
        pl.semaphore_signal(barrier, inc=1, device_id={'ep': (me + step) % ep}, device_id_type=MESH)
    for side in range(2):
        pl.semaphore_signal(barrier, inc=1, device_id={'pp': next_stage, 'ep': 2 * chip + side}, device_id_type=MESH)
        pl.semaphore_signal(barrier, inc=1, device_id={'pp': prev_stage, 'ep': 2 * chip + side}, device_id_type=MESH)
    pl.semaphore_wait(barrier, ep - 1 + 4)

    for step in range(1, ep):
        meta_copy(step).start()
    for j in range(blocks):
        swap_rows(j).start()
    swap_resid.start()

    def build_gates(role):
        table = jnp.transpose(meta[owners[role]])
        wanted = (lax.broadcasted_iota(jnp.int32, (tokens, chip_rows), 1) + chip * chip_rows).astype(jnp.float32)
        total = jnp.zeros((tokens, chip_rows), jnp.float32)
        for t in range(top):
            total = total + jnp.where(table[:, t:t + 1] == wanted, table[:, top + t:top + t + 1], 0.0)
        high = total.astype(jnp.bfloat16)
        rest = total - high.astype(jnp.float32)
        mid = rest.astype(jnp.bfloat16)
        low = (rest - mid.astype(jnp.float32)).astype(jnp.bfloat16)
        for t in range(chunks):
            for i, term in enumerate((high, mid, low)):
                gate_mats[role, t, i * CHUNK:(i + 1) * CHUNK] = term[t * CHUNK:(t + 1) * CHUNK]

    def contribution(role, s):
        slot0 = pl.multiple_of(owners[role] * cap_dev, cap_dev)
        rows = pool[s % blocks, :, pl.ds(slot0, cap_dev), :].reshape(chip_rows, COLS)
        parts = jnp.dot(gate_mats[role, s // blocks], rows, preferred_element_type=jnp.float32)
        return parts[2 * CHUNK:] + parts[CHUNK:2 * CHUNK] + parts[:CHUNK]

    def leaf(kind, s):
        @pl.when(s >= 2)
        def _():
            ring_copy(kind, s - 2).wait_send()

        send_v[kind, s % 2] = contribution(kind, s)
        ring_copy(kind, s).start()

    def forward(kind, s):
        own = contribution(kind, s)

        @pl.when(s >= 2)
        def _():
            ring_copy(kind, s - 2).wait_send()

        ring_copy(kind - 4, s).wait_recv()
        send_v[kind, s % 2] = own + recv_v[kind - 4, s]
        ring_copy(kind, s).start()

    def finish(side, s):
        near, far = ((3, 4), (2, 5))[side]
        own = contribution(6 + side, s)

        @pl.when(s >= 2)
        def _():
            y_copy(side, s - 2).wait_send()

        ring_copy(near, s).wait_recv()
        ring_copy(far, s).wait_recv()
        resid = resid_v[side, span(s // blocks), lanes_at(s % blocks * COLS)].astype(jnp.float32)
        ysend_v[side, s % 2] = (resid + (own + recv_v[near, s] + recv_v[far, s])).astype(jnp.bfloat16)
        y_copy(side, s).start()

    def pass_on(s):
        for part in range(2):
            pltpu.make_async_copy(ysend_v.at[0, 0], ysend_v.at[0, 0], y_rs.at[part, s]).wait()
            y_relay(part, s).start()

    def take(s):
        @pl.when(s % blocks == 0)
        def _():
            square_v[...] = jnp.zeros_like(square_v)

        for part in range(2):
            y_relay(part, s).wait_recv()
            for seq in range(2):
                piece = y_v[seq, part * blocks + s % blocks, span(s // blocks)].astype(jnp.float32)
                square_v[seq] += piece * piece

    def normalize(t):
        for seq in range(2):
            mean = jnp.sum(square_v[seq], axis=-1, keepdims=True) / width
            inv_rms = lax.rsqrt(mean + NORM_EPS)
            for i in range(depth):
                cols = slice(i * COLS, (i + 1) * COLS)
                x_v[seq * CHUNK:(seq + 1) * CHUNK, cols] = (
                    y_v[seq, i, span(t)].astype(jnp.float32) * inv_rms * scale_ref[:, cols]).astype(jnp.bfloat16)

    def fetch(pair):
        for which in range(3):
            start_all(qkv_copies(which, pair, slot_of(which, pair)))

    def wait_pair(i, pair, t):
        @pl.when(jnp.logical_or(t == 0, i >= RING_PAIRS))
        def _():
            for which in range(3):
                wait_all(qkv_copies(which, 0, slot_of(which, pair)))

    def refill(pair, t):
        odd = t % 2
        later = pair + (1 - 2 * odd) * RING_PAIRS

        @pl.when(jnp.logical_and(later >= 0, later < pairs))
        def _():
            fetch(later)

    def project(pair, t):
        for which in range(3):
            slot = slot_of(which, pair)
            weight = jnp.concatenate([heads_v[slot, i].reshape(width, head_dim) for i in range(2)], axis=1)
            product = jnp.dot(x_v[...], weight, preferred_element_type=jnp.float32).astype(jnp.bfloat16)
            if which == 0:
                q_v[pair % 2] = product
            else:
                for seq in range(2):
                    kv_v[which - 1, pair, seq, span(t)] = product[seq * CHUNK:(seq + 1) * CHUNK]

    def attend(pair, t):
        causal = (lax.broadcasted_iota(jnp.int32, (CHUNK, tokens), 0) + t * CHUNK
                  >= lax.broadcasted_iota(jnp.int32, (CHUNK, tokens), 1))
        mixed = []
        for seq in range(2):
            for i in range(2):
                lanes = slice(i * head_dim, (i + 1) * head_dim)
                q = q_v[pair % 2, seq * CHUNK:(seq + 1) * CHUNK, lanes]
                k, v = kv_v[0, pair, seq, :, lanes], kv_v[1, pair, seq, :, lanes]
                scores = lax.dot_general(q, k, (((1,), (1,)), ((), ())), preferred_element_type=jnp.float32) * head_dim ** -0.5
                scores = jnp.where(causal, scores, -1e30)
                exps = jnp.exp(scores - jnp.max(scores, axis=-1, keepdims=True))
                sums = jnp.sum(exps, axis=-1, keepdims=True)
                mixed.append((jnp.dot(exps.astype(jnp.bfloat16), v, preferred_element_type=jnp.float32) / sums).astype(jnp.bfloat16))
        return mixed

    def store_mixed(pair, t, mixed):
        for seq in range(2):
            for i in range(2):
                mix_v[core * pairs + pair, seq, span(t), i * head_dim:(i + 1) * head_dim] = mixed[2 * seq + i]
        mix_copy(pair, t).start()

    for step in range(1, ep):
        meta_copy(step).wait_recv()

    def ring_step(s, carry):
        @pl.when(s < steps)
        def _():
            @pl.when(s < blocks)
            def _():
                local_rows(s).wait()
                swap_rows(s).wait_recv()

            for kind in range(4):
                @pl.when(s == 0)
                def _():
                    build_gates(kind)

                leaf(kind, s)

        @pl.when(s == 0)
        def _():
            for role in range(4, 8):
                build_gates(role)
            local_resid.wait()
            swap_resid.wait_recv()
            kv_v[...] = jnp.zeros_like(kv_v)

        for which in range(3):
            @pl.when(jnp.logical_and(s % 3 == which, s < 3 * RING_PAIRS))
            def _():
                start_all(qkv_copies(which, s // 3, slot_of(which, s // 3)))

        @pl.when(jnp.logical_and(s >= 1, s < steps + 1))
        def _():
            forward(4, s - 1)
            forward(5, s - 1)

        lag = s % blocks - 4

        @pl.when(jnp.logical_and(jnp.logical_and(s >= blocks, s < steps), lag >= 0))
        def _():
            def one_pair(i, carry):
                t = s // blocks - 1
                odd = t % 2
                pair = odd * (pairs - 1) + (1 - 2 * odd) * i
                wait_pair(i, pair, t)
                project(pair, t)
                refill(pair, t)
                store_mixed(pair, t, attend(pair, t))
                return carry

            lax.fori_loop(3 * lag, jnp.minimum(3 * lag + 3, pairs), one_pair, 0)

        @pl.when(jnp.logical_and(s >= 2, s < steps + 2))
        def _():
            finish(0, s - 2)
            finish(1, s - 2)

            @pl.when(s - 2 >= steps - blocks)
            def _():
                start_all(out_copies(s - 2 - (steps - blocks)))

        @pl.when(jnp.logical_and(s >= 3, s < steps + 3))
        def _():
            pass_on(s - 3)

        @pl.when(s >= 4)
        def _():
            take(s - 4)

        @pl.when(jnp.logical_and(s >= blocks, s % blocks == 3))
        def _():
            normalize(s // blocks - 1)

        return carry

    lax.fori_loop(0, steps + 4, ring_step, 0)

    last = chunks - 1
    flip = last % 2

    def nth(i):
        return pairs - 1 - i if flip else i

    wait_pair(0, nth(0), last)
    project(nth(0), last)
    refill(nth(0), last)

    def pair_step(i, carry):
        wait_pair(i, nth(i), last)
        mixed = attend(nth(i - 1), last)
        project(nth(i), last)
        store_mixed(nth(i - 1), last, mixed)
        refill(nth(i), last)
        return carry

    lax.fori_loop(1, pairs, pair_step, 0)
    store_mixed(nth(pairs - 1), last, attend(nth(pairs - 1), last))

    for t in range(chunks):
        for pair in range(pairs):
            mix_copy(pair, t).wait_recv()

    def store_z(n):
        return pltpu.make_async_copy(z_v.at[n % 2, core], z_out.at[:, lanes_at(core * half + n * COLS)], z_sem.at[n])

    def send_z(n):
        return pltpu.make_async_remote_copy(
            src_ref=z_v.at[n % 2, 1 - core], dst_ref=z_out.at[:, lanes_at(core * half + n * COLS)],
            send_sem=zr_ss.at[n], recv_sem=zr_rs.at[n], device_id={'ep': partner}, device_id_type=MESH)

    def out_step(n, carry):
        wait_all(out_copies(n))
        mixed = jnp.concatenate([mix_v[i].reshape(2 * tokens, COLS) for i in range(depth)], axis=1)
        weight = pool[n, 0:depth].reshape(width, COLS)
        product = jnp.dot(mixed, weight, preferred_element_type=jnp.float32).astype(jnp.bfloat16)

        @pl.when(n >= 2)
        def _():
            store_z(n - 2).wait()
            send_z(n - 2).wait_send()

        for seq in range(2):
            resid = y_v[seq, core * blocks + n].astype(jnp.float32)
            z_v[n % 2, seq] = (resid + product[seq * tokens:(seq + 1) * tokens].astype(jnp.float32)).astype(jnp.bfloat16)
        send_z(n).start()
        store_z(n).start()
        return carry

    lax.fori_loop(0, blocks, out_step, 0)
    for n in range(blocks - 2, blocks):
        store_z(n).wait()
        send_z(n).wait_send()
    for n in range(blocks):
        send_z(n).wait_recv()
    for step in range(1, ep):
        meta_copy(step).wait_send()
    for j in range(blocks):
        swap_rows(j).wait_send()
    swap_resid.wait_send()
    for t in range(chunks):
        for pair in range(pairs):
            mix_copy(pair, t).wait_send()
    for s in range(steps):
        for part in range(2):
            y_relay(part, s).wait_send()
    for s in range(steps - 2, steps):
        for kind in range(6):
            ring_copy(kind, s).wait_send()
        for side in range(2):
            y_copy(side, s).wait_send()


def combine_and_attend(ep, pp, expert_out, expert_ids, slot_ids, gate_vals, residual, norm_scale, w_query, w_key, w_value, w_out):
    experts, cap, width = expert_out.shape
    tokens, top = expert_ids.shape
    heads, head_dim = w_query.shape[1:]
    sizes = (ep, pp, experts, cap, width, tokens, top, heads, head_dim)
    half = width // 2
    blocks = half // COLS
    chunks = tokens // CHUNK
    steps = chunks * blocks
    depth = width // COLS
    pairs = heads // 4
    chip_rows = 2 * experts * cap // ep
    any_spec = pl.BlockSpec(memory_space=pl.ANY)
    vmem_spec = pl.BlockSpec(memory_space=pltpu.VMEM)
    dma = pltpu.SemaphoreType.DMA

    def by_head(weights):
        return jnp.swapaxes(weights, 0, 1).reshape(heads, depth, COLS, head_dim)

    return pl.pallas_call(
        functools.partial(layer_kernel, sizes),
        out_shape=jax.ShapeDtypeStruct((tokens, width), jnp.bfloat16),
        in_specs=[any_spec, vmem_spec, vmem_spec, vmem_spec, any_spec, vmem_spec] + [any_spec] * 4,
        out_specs=any_spec,
        scratch_shapes=[
            pltpu.VMEM((blocks, 2 * experts, cap, COLS), jnp.bfloat16),
            pltpu.VMEM((3 * RING_PAIRS, 2, depth, COLS, head_dim), jnp.bfloat16),
            pltpu.VMEM((2, tokens, half), jnp.bfloat16),
            pltpu.VMEM((ep, 2 * top, tokens), jnp.float32),
            pltpu.VMEM((8, chunks, 3 * CHUNK, chip_rows), jnp.bfloat16),
            pltpu.VMEM((6, 2, CHUNK, COLS), jnp.float32),
            pltpu.VMEM((6, steps, CHUNK, COLS), jnp.float32),
            pltpu.VMEM((2, 2, CHUNK, COLS), jnp.bfloat16),
            pltpu.VMEM((2, depth, tokens, COLS), jnp.bfloat16),
            pltpu.VMEM((2, CHUNK, COLS), jnp.float32),
            pltpu.VMEM((2 * CHUNK, width), jnp.bfloat16),
            pltpu.VMEM((2, 2 * CHUNK, COLS), jnp.bfloat16),
            pltpu.VMEM((2, pairs, 2, tokens, COLS), jnp.bfloat16),
            pltpu.VMEM((2 * pairs, 2, tokens, COLS), jnp.bfloat16),
            pltpu.VMEM((2, 2, tokens, COLS), jnp.bfloat16),
            dma((blocks,)), dma((blocks,)), dma((blocks,)), dma, dma, dma, dma((ep - 1,)), dma((ep - 1,)),
            dma((6, steps)), dma((6, steps)), dma((2, steps)), dma((2, steps)), dma((2, steps)), dma((2, steps)),
            dma((chunks, pairs)), dma((chunks, pairs)), dma((3 * RING_PAIRS, 2)), dma((blocks, 2)), dma((blocks,)), dma((blocks,)), dma((blocks,)),
        ],
        compiler_params=pltpu.CompilerParams(collective_id=0, has_side_effects=True, vmem_limit_bytes=67043328),
    )(expert_out, expert_ids.T, slot_ids.T, gate_vals.T, residual, norm_scale[None],
      by_head(w_query), by_head(w_key), by_head(w_value), w_out.reshape(depth, COLS, width))


def solution(mesh):
    ep_size = mesh.shape['ep']
    pp_size = mesh.shape['pp']
    token_spec = P(('data', 'pp'), 'ep', None, None)
    weight_spec = P('pp', None, None, None)

    def body(expert_out, expert_ids, slot_ids, gate_vals, residual, norm_scale, w_query, w_key, w_value, w_out):
        result = combine_and_attend(
            ep_size, pp_size, expert_out[0], expert_ids[0, 0], slot_ids[0, 0], gate_vals[0, 0], residual[0, 0],
            norm_scale[0], w_query[0], w_key[0], w_value[0], w_out[0])
        return result[None, None]

    return jax.shard_map(body, mesh=mesh, in_specs=(token_spec, token_spec, token_spec, token_spec, token_spec, P('pp', None), weight_spec, weight_spec, weight_spec, weight_spec), out_specs=token_spec, check_vma=False)
```

```python
import functools

import jax
import jax.numpy as jnp
from jax import lax
from jax.experimental import pallas as pl
from jax.experimental.pallas import tpu as pltpu
from jax.sharding import PartitionSpec as P

NORM_EPS = 1e-6
COLS = 256
SLOTS = 19
MESH = pl.DeviceIdType.MESH


def layer_kernel(sizes, o_hbm, ids, slots, gates, h_hbm, scale_ref, wq_hbm, wk_hbm, wv_hbm, wo_hbm, z_out, y_out,
                 pool, resid_v, meta, gate_mats, send_v, recv_v, ysend_v, y_v, square_v, x_v, qkv_v, mix_v, z_v,
                 rows_loc, rows_ss, rows_rs, res_loc, res_ss, res_rs, meta_ss, meta_rs,
                 ring_ss, ring_rs, y_ss, y_rs, w_sem, z_sem, yo_sem):
    ep, pp, experts, cap, width, tokens, top, heads, head_dim = sizes
    chips = ep // 2
    half = width // 2
    blocks = half // COLS
    cap_dev = cap // ep
    chip_rows = 2 * experts * cap_dev
    me = lax.axis_index('ep')
    stage = lax.axis_index('pp')
    chip, core = me // 2, me % 2
    partner = chip * 2 + (1 - core)
    ahead, behind, across = (chip + 1) % chips, (chip + chips - 1) % chips, (chip + 2) % chips
    next_stage, prev_stage = (stage + 1) % pp, (stage + pp - 1) % pp
    right, left = 2 * ahead + core, 2 * behind + core
    owners = (2 * across, 2 * across + 1, 2 * ahead + 1, 2 * behind, 2 * ahead, 2 * behind + 1, 2 * chip, 2 * chip + 1)

    def local_rows(j):
        cols = pl.ds(pl.multiple_of(core * half + j * COLS, COLS), COLS)
        return pltpu.make_async_copy(o_hbm.at[:, :, cols], pool.at[j, pl.ds(core * experts, experts)], rows_loc.at[j])

    def swap_rows(j):
        cols = pl.ds(pl.multiple_of((1 - core) * half + j * COLS, COLS), COLS)
        return pltpu.make_async_remote_copy(
            src_ref=o_hbm.at[:, :, cols], dst_ref=pool.at[j, pl.ds(core * experts, experts)],
            send_sem=rows_ss.at[j], recv_sem=rows_rs.at[j], device_id={'ep': partner}, device_id_type=MESH)

    own_cols = pl.ds(pl.multiple_of(core * half, COLS), half)
    other_cols = pl.ds(pl.multiple_of((1 - core) * half, COLS), half)
    local_resid = pltpu.make_async_copy(h_hbm.at[:, own_cols], resid_v.at[core], res_loc)
    swap_resid = pltpu.make_async_remote_copy(
        src_ref=h_hbm.at[:, other_cols], dst_ref=resid_v.at[core],
        send_sem=res_ss, recv_sem=res_rs, device_id={'ep': partner}, device_id_type=MESH)

    def meta_copy(step):
        return pltpu.make_async_remote_copy(
            src_ref=meta.at[me], dst_ref=meta.at[me], send_sem=meta_ss.at[step - 1], recv_sem=meta_rs.at[step - 1],
            device_id={'ep': (me + step) % ep}, device_id_type=MESH)

    def part(hf):
        return slice(hf * tokens // 2, (hf + 1) * tokens // 2)

    def ring_copy(kind, j, hf=0):
        target = right if kind % 2 == 0 else left
        rows = part(hf) if kind >= 4 else slice(0, tokens)
        return pltpu.make_async_remote_copy(
            src_ref=send_v.at[kind, j % 2, rows], dst_ref=recv_v.at[kind, j, rows], send_sem=ring_ss.at[kind + 2 * hf, j],
            recv_sem=ring_rs.at[kind + 2 * hf, j], device_id={'ep': target}, device_id_type=MESH)

    def y_copy(side, j, hf):
        return pltpu.make_async_remote_copy(
            src_ref=ysend_v.at[side, j % 2, part(hf)], dst_ref=y_v.at[core * blocks + j, part(hf)], send_sem=y_ss.at[hf, side, j],
            recv_sem=y_rs.at[hf, core * blocks + j], device_id={'pp': next_stage, 'ep': 2 * chip + side}, device_id_type=MESH)

    pairs = heads // 2
    depth = width // COLS
    n_slots = pool.shape[0]
    early = n_slots - blocks
    units = 3 * pairs + width // COLS

    def qkv_copies(which, pair, slot):
        w_hbm = (wq_hbm, wk_hbm, wv_hbm)[which]
        return [pltpu.make_async_copy(w_hbm.at[2 * pair + i], pool.at[slot, 0:depth, :, i * head_dim:(i + 1) * head_dim],
                                      w_sem.at[slot, i]) for i in range(2)]

    def out_copies(n, slot):
        cols = pl.ds(pl.multiple_of(n * COLS, COLS), COLS)
        mid = depth // 2
        return [pltpu.make_async_copy(wo_hbm.at[i * mid:(i + 1) * mid, :, cols], pool.at[slot, i * mid:(i + 1) * mid],
                                      w_sem.at[slot, i]) for i in range(2)]

    def slot_of(unit):
        return (unit + blocks) % n_slots

    def start_all(copies):
        for copy in copies:
            copy.start()

    def start_unit(unit, which):
        @pl.when(unit < 3 * pairs)
        def _():
            start_all(qkv_copies(which, unit // 3, slot_of(unit)))

        @pl.when(jnp.logical_and(unit >= 3 * pairs, unit < units))
        def _():
            start_all(out_copies(unit - 3 * pairs, slot_of(unit)))

    def start_any(unit):
        for which in range(3):
            @pl.when(unit % 3 == which)
            def _():
                start_unit(unit, which)

    def square_piece(j):
        for side in range(2):
            piece = y_v[side * blocks + j].astype(jnp.float32)
            square_v[...] += piece * piece

    def store_y(i):
        return pltpu.make_async_copy(y_v.at[i], y_out.at[:, pl.ds(pl.multiple_of(i * COLS, COLS), COLS)], yo_sem.at[i])

    def wait_y(j):
        for side in range(2):
            for hf in range(2):
                piece = y_v.at[side * blocks + j, part(hf)]
                pltpu.make_async_copy(piece, piece, y_rs.at[hf, side * blocks + j]).wait()
            store_y(side * blocks + j).start()

    for j in range(blocks):
        local_rows(j).start()
    local_resid.start()
    square_v[...] = jnp.zeros_like(square_v)
    row_ids = jnp.where(slots[...] >= 0, ids[...] * cap_dev + slots[...] - me * cap_dev, -1)
    meta[me, 0:top, :] = row_ids.astype(jnp.float32)
    meta[me, top:2 * top, :] = gates[...]

    barrier = pltpu.get_barrier_semaphore()
    for step in range(1, ep):
        pl.semaphore_signal(barrier, inc=1, device_id={'ep': (me + step) % ep}, device_id_type=MESH)
    for side in range(2):
        pl.semaphore_signal(barrier, inc=1, device_id={'pp': next_stage, 'ep': 2 * chip + side}, device_id_type=MESH)
        pl.semaphore_signal(barrier, inc=1, device_id={'pp': prev_stage, 'ep': 2 * chip + side}, device_id_type=MESH)
    pl.semaphore_wait(barrier, ep - 1 + 4)

    for step in range(1, ep):
        meta_copy(step).start()
    for j in range(blocks):
        swap_rows(j).start()
    swap_resid.start()

    def build_gates(role):
        table = jnp.transpose(meta[owners[role]])
        wanted = (lax.broadcasted_iota(jnp.int32, (tokens, chip_rows), 1) + chip * chip_rows).astype(jnp.float32)
        total = jnp.zeros((tokens, chip_rows), jnp.float32)
        for t in range(top):
            total = total + jnp.where(table[:, t:t + 1] == wanted, table[:, top + t:top + t + 1], 0.0)
        high = total.astype(jnp.bfloat16)
        rest = total - high.astype(jnp.float32)
        mid = rest.astype(jnp.bfloat16)
        low = (rest - mid.astype(jnp.float32)).astype(jnp.bfloat16)
        gate_mats[role, 0:tokens] = high
        gate_mats[role, tokens:2 * tokens] = mid
        gate_mats[role, 2 * tokens:3 * tokens] = low

    def contribution(role, j):
        slot0 = pl.multiple_of(owners[role] * cap_dev, cap_dev)
        rows = pool[j, :, pl.ds(slot0, cap_dev), :].reshape(chip_rows, COLS)
        parts = jnp.dot(gate_mats[role], rows, preferred_element_type=jnp.float32)
        return parts[2 * tokens:] + parts[tokens:2 * tokens] + parts[:tokens]

    def finish(j):
        cols = pl.ds(pl.multiple_of(j * COLS, COLS), COLS)
        owns = [contribution(6 + side, j) for side in range(2)]

        @pl.when(j >= 2)
        def _():
            for side in range(2):
                for hf in range(2):
                    y_copy(side, j - 2, hf).wait_send()

        for hf in range(2):
            for side, (near, far) in enumerate(((3, 4), (2, 5))):
                if hf == 0:
                    ring_copy(near, j).wait_recv()
                ring_copy(far, j, hf).wait_recv()
                resid = resid_v[side, part(hf), cols].astype(jnp.float32)
                total = resid + (owns[side][part(hf)] + recv_v[near, j, part(hf)] + recv_v[far, j, part(hf)])
                ysend_v[side, j % 2, part(hf)] = total.astype(jnp.bfloat16)
                y_copy(side, j, hf).start()

    for step in range(1, ep):
        meta_copy(step).wait_recv()

    def block_step(j, carry):
        local_rows(j).wait()
        swap_rows(j).wait_recv()

        for kind in range(4):
            @pl.when(j == 0)
            def _():
                build_gates(kind)

            @pl.when(j >= 2)
            def _():
                ring_copy(kind, j - 2).wait_send()

            send_v[kind, j % 2] = contribution(kind, j)
            ring_copy(kind, j).start()

        @pl.when(j == 0)
        def _():
            for role in range(4, 8):
                build_gates(role)
            local_resid.wait()
            swap_resid.wait_recv()
            for unit in range(early):
                start_all(qkv_copies(unit % 3, unit // 3, slot_of(unit)))

        @pl.when(j > 0)
        def _():
            finish(j - 1)
            start_any(early + j - 1)

        @pl.when(j > 1)
        def _():
            wait_y(j - 2)
            square_piece(j - 2)

        for kind in (4, 5):
            own = contribution(kind, j)

            @pl.when(j >= 2)
            def _():
                for hf in range(2):
                    ring_copy(kind, j - 2, hf).wait_send()

            ring_copy(kind - 4, j).wait_recv()
            send_v[kind, j % 2] = own + recv_v[kind - 4, j]
            for hf in range(2):
                ring_copy(kind, j, hf).start()
        return carry

    lax.fori_loop(0, blocks, block_step, 0)
    finish(blocks - 1)

    start_any(early + blocks - 1)
    for j in (blocks - 2, blocks - 1):
        wait_y(j)
        square_piece(j)
    mean = jnp.sum(square_v[...], axis=-1, keepdims=True) / width
    inv_rms = lax.rsqrt(mean + NORM_EPS)
    for i in range(depth):
        cols = slice(i * COLS, (i + 1) * COLS)
        x_v[:, cols] = (y_v[i].astype(jnp.float32) * inv_rms * scale_ref[:, cols]).astype(jnp.bfloat16)

    def wait_unit(unit):
        for copy in out_copies(0, slot_of(unit)):
            copy.wait()

    def weight(unit):
        return pool[slot_of(unit), 0:depth].reshape(width, COLS)

    def project(pair):
        for which in range(3):
            product = jnp.dot(x_v[...], weight(3 * pair + which), preferred_element_type=jnp.float32)
            qkv_v[pair % 2, which] = product.astype(jnp.bfloat16)

    causal = lax.broadcasted_iota(jnp.int32, (tokens, tokens), 0) >= lax.broadcasted_iota(jnp.int32, (tokens, tokens), 1)

    def attend(pair):
        mixed = []
        for i in range(2):
            lanes = slice(i * head_dim, (i + 1) * head_dim)
            q, k, v = (qkv_v[pair % 2, which, :, lanes] for which in range(3))
            scores = lax.dot_general(q, k, (((1,), (1,)), ((), ())), preferred_element_type=jnp.float32) * head_dim ** -0.5
            scores = jnp.where(causal, scores, -1e30)
            exps = jnp.exp(scores - jnp.max(scores, axis=-1, keepdims=True))
            sums = jnp.sum(exps, axis=-1, keepdims=True)
            mixed.append((jnp.dot(exps.astype(jnp.bfloat16), v, preferred_element_type=jnp.float32) / sums).astype(jnp.bfloat16))
        return mixed

    def store_mixed(pair, mixed):
        for i in range(2):
            mix_v[:, pl.ds(pl.multiple_of(pair * COLS + i * head_dim, head_dim), head_dim)] = mixed[i]

    def refill(pair):
        for which in range(3):
            start_unit(3 * pair + which + n_slots, (which + n_slots) % 3)

    def wait_pair(pair):
        for which in range(3):
            wait_unit(3 * pair + which)

    wait_pair(0)
    project(0)
    refill(0)

    def pair_step(pair, carry):
        wait_pair(pair)
        mixed = attend(pair - 1)
        project(pair)
        store_mixed(pair - 1, mixed)
        refill(pair)
        return carry

    lax.fori_loop(1, pairs, pair_step, 0)
    store_mixed(pairs - 1, attend(pairs - 1))

    def store_z(n):
        return pltpu.make_async_copy(z_v.at[n % 2], z_out.at[:, pl.ds(pl.multiple_of(n * COLS, COLS), COLS)], z_sem.at[n % 2])

    def out_step(n, carry):
        wait_unit(3 * pairs + n)
        product = jnp.dot(mix_v[...], weight(3 * pairs + n), preferred_element_type=jnp.float32).astype(jnp.bfloat16)

        @pl.when(n >= 2)
        def _():
            store_z(n - 2).wait()

        z_v[n % 2] = product
        store_z(n).start()
        start_unit(3 * pairs + n + n_slots, 0)
        return carry

    lax.fori_loop(0, depth, out_step, 0)
    store_z(depth - 2).wait()
    store_z(depth - 1).wait()
    for i in range(depth):
        store_y(i).wait()
    for step in range(1, ep):
        meta_copy(step).wait_send()
    for j in range(blocks):
        swap_rows(j).wait_send()
    swap_resid.wait_send()
    for j in range(blocks - 2, blocks):
        for kind in range(4):
            ring_copy(kind, j).wait_send()
        for hf in range(2):
            for side in range(2):
                ring_copy(4 + side, j, hf).wait_send()
                y_copy(side, j, hf).wait_send()


def combine_and_attend(ep, pp, expert_out, expert_ids, slot_ids, gate_vals, residual, norm_scale, w_query, w_key, w_value, w_out):
    experts, cap, width = expert_out.shape
    tokens, top = expert_ids.shape
    heads, head_dim = w_query.shape[1:]
    sizes = (ep, pp, experts, cap, width, tokens, top, heads, head_dim)
    blocks = width // 2 // COLS
    depth = width // COLS
    chip_rows = 2 * experts * cap // ep
    any_spec = pl.BlockSpec(memory_space=pl.ANY)
    vmem_spec = pl.BlockSpec(memory_space=pltpu.VMEM)
    dma = pltpu.SemaphoreType.DMA

    def by_head(weights):
        return jnp.swapaxes(weights, 0, 1).reshape(heads, depth, COLS, head_dim)

    return pl.pallas_call(
        functools.partial(layer_kernel, sizes),
        out_shape=[jax.ShapeDtypeStruct((tokens, width), jnp.bfloat16)] * 2,
        in_specs=[any_spec, vmem_spec, vmem_spec, vmem_spec, any_spec, vmem_spec] + [any_spec] * 4,
        out_specs=[any_spec, any_spec],
        scratch_shapes=[
            pltpu.VMEM((SLOTS, 2 * experts, cap, COLS), jnp.bfloat16),
            pltpu.VMEM((2, tokens, width // 2), jnp.bfloat16),
            pltpu.VMEM((ep, 2 * top, tokens), jnp.float32),
            pltpu.VMEM((8, 3 * tokens, chip_rows), jnp.bfloat16),
            pltpu.VMEM((6, 2, tokens, COLS), jnp.float32),
            pltpu.VMEM((6, blocks, tokens, COLS), jnp.float32),
            pltpu.VMEM((2, 2, tokens, COLS), jnp.bfloat16),
            pltpu.VMEM((2 * blocks, tokens, COLS), jnp.bfloat16),
            pltpu.VMEM((tokens, COLS), jnp.float32),
            pltpu.VMEM((tokens, width), jnp.bfloat16),
            pltpu.VMEM((2, 3, tokens, COLS), jnp.bfloat16),
            pltpu.VMEM((tokens, heads * head_dim), jnp.bfloat16),
            pltpu.VMEM((2, tokens, COLS), jnp.bfloat16),
            dma((blocks,)), dma((blocks,)), dma((blocks,)), dma, dma, dma, dma((ep - 1,)), dma((ep - 1,)),
            dma((8, blocks)), dma((8, blocks)), dma((2, 2, blocks)), dma((2, 2 * blocks)), dma((SLOTS, 2)), dma((2,)), dma((depth,)),
        ],
        compiler_params=pltpu.CompilerParams(collective_id=0, has_side_effects=True, vmem_limit_bytes=67043328),
    )(expert_out, expert_ids.T, slot_ids.T, gate_vals.T, residual, norm_scale[None],
      by_head(w_query), by_head(w_key), by_head(w_value), w_out.reshape(heads * head_dim // COLS, COLS, width))


def solution(mesh):
    ep_size = mesh.shape['ep']
    pp_size = mesh.shape['pp']
    token_spec = P(('data', 'pp'), 'ep', None, None)
    weight_spec = P('pp', None, None, None)

    def body(expert_out, expert_ids, slot_ids, gate_vals, residual, norm_scale, w_query, w_key, w_value, w_out):
        projected, arrived = combine_and_attend(
            ep_size, pp_size, expert_out[0], expert_ids[0, 0], slot_ids[0, 0], gate_vals[0, 0], residual[0, 0],
            norm_scale[0], w_query[0], w_key[0], w_value[0], w_out[0])
        result = (arrived.astype(jnp.float32) + projected.astype(jnp.float32)).astype(jnp.bfloat16)
        return result[None, None]

    return jax.shard_map(body, mesh=mesh, in_specs=(token_spec, token_spec, token_spec, token_spec, token_spec, P('pp', None), weight_spec, weight_spec, weight_spec, weight_spec), out_specs=token_spec, check_vma=False)
```
